32 devices in a mesh: group: 8 (over z, y), peer: 4 (over x, core).
Axes of the slice: x: 2, y: 2, z: 4, core: 2. Of those that a mesh axis runs over, the one named last changes fastest.
Arguments:
- features: float32 [128, 64, 384], P('group', 'peer'), may hold values from -6 to 6
- image_of_row: int32 [8], replicated, may hold values from 0 to 3, never falling along the last dimension, each value on 1 to 4 neighbouring positions
- llm_peer: int32 [32, 1], P(('group', 'peer')), may hold values from 0 to 3, as said below
- token_grads: float32 [64, 64, 384], P(('group', 'peer')), may hold values from -6 to 6
- dw_weight: float32 [49, 384], replicated, may hold values from -0.875 to 0.875
- dw_bias: float32 [384], replicated, may hold values from -3 to 3
- ln_gain: float32 [384], replicated, may hold values from 0.1 to 1.9
- ln_bias: float32 [384], replicated, may hold values from -3 to 3
- w_in: bfloat16 [384, 1536], replicated, may hold values from -0.3125 to 0.3125
- b_in: float32 [1536], replicated, may hold values from -3 to 3
- w_out: bfloat16 [1536, 384], replicated, may hold values from -0.15625 to 0.15625
- b_out: float32 [384], replicated, may hold values from -3 to 3
- layer_scale: float32 [384], replicated, may hold values from 0.3 to 1
- comp_weight: bfloat16 [9, 384, 384], replicated, may hold values from -0.109375 to 0.109375
- comp_bias: float32 [384], replicated, may hold values from -3 to 3
Outputs:
- llm_tokens: float32 [64, 64, 384], P(('group', 'peer'))
- feature_grads: float32 [128, 64, 384], P('group', 'peer')
The draws below stay inside these ranges and needn't reach their ends.
Inputs may be any that keep to these rules, and one draw needn't show every extreme that they name: `llm_peer`: the 1 tiles of one device go to 1 different peers of its group; each peer receives at most 2 tiles of its tile row, and in tile row 0 some peer receives exactly 2. `image_of_row`: Non-decreasing along tile rows; each image spans 1 to 4 consecutive tile rows.
All inputs are finite; a program needn't handle non-finite values.
Results may differ from the reference program's by a relative error of at most 0.005.
Values sent between devices are 32-bit elements; how exact they have to be, the bound alone decides.
A program may use at most 64 MiB of HBM per device.

```python
import math
import jax
import jax.numpy as jnp
import numpy as np
from jax import lax

C = 384
HID = 1536
SIDE = 16
TPD = 1
CAP = 2
POOLED = 8
IMAGES = 4
N_GROUP = 8
N_PEER = 4


def draw_llm_peer(key, part):
    order_key = jax.random.fold_in(key, 11)
    law_key = jax.random.fold_in(key, 12)
    row_keys = jax.random.split(order_key, N_GROUP)
    orders = jax.vmap(lambda k: jax.random.permutation(k, N_PEER))(row_keys).astype(jnp.int32)
    position = jnp.argsort(orders, axis=1, stable=True).astype(jnp.int32)
    lawbit = jax.random.randint(law_key, (N_GROUP,), 0, 2).astype(jnp.int32)
    lawbit = lawbit.at[0].set(1)
    tile_num = jnp.arange(TPD, dtype=jnp.int32)
    half_count = N_PEER // 2
    skewed = (position[:, :, None] // 2 + tile_num[None, None, :]) % half_count
    even = (position[:, :, None] + tile_num[None, None, :]) % N_PEER
    chosen = jnp.where(lawbit[:, None, None] == 1, skewed, even)
    dest = jnp.take_along_axis(orders[:, None, :], chosen.reshape(N_GROUP, 1, N_PEER * TPD), axis=2)
    return dest.reshape(N_GROUP * N_PEER * TPD, 1).astype(jnp.int32)


def block_scale(stream_key, dims, cuts, least, top_value):
    factor_of, own = 1.0, jax.random.fold_in(stream_key, 6)
    for axis_at, shards_of in cuts:
        steps = jnp.exp(jax.random.uniform(jax.random.fold_in(own, axis_at), (shards_of,), jnp.float32, least / len(cuts), top_value / len(cuts)))
        factor_of = factor_of * jnp.repeat(steps, dims[axis_at] // shards_of).reshape([-1 if axis == axis_at else 1 for axis in range(len(dims))])
    return factor_of


def length_profile(amount, total, limit, lean):
    loads = [(1 << 20) // math.isqrt(rank ** lean) + 1 for rank in range(2, amount + 1)]
    rest, counts = total - limit - (amount - 1), [1] * (amount - 1)
    while rest > 0:
        movable = [i for i in range(amount - 1) if counts[i] < limit]
        mass, budget = sum([loads[i] for i in movable]), rest
        for i in movable:
            more = min(limit - counts[i], max(1, budget * loads[i] // mass), rest)
            counts[i] = counts[i] + more
            rest = rest - more
    return np.array([limit] + counts)


def ragged(own_key, count, total, reach, skew):
    if count == 2:
        one = jax.random.randint(own_key, (), max(1, total - reach), min(reach, total - 1) + 1)
        return jnp.stack([one, total - one])
    tallies = jnp.asarray(length_profile(count, total, reach, skew), jnp.int32)
    couples = (count - 1) // 2
    source_of, sink = tallies[1:1 + 2 * couples:2], tallies[2:2 + 2 * couples:2]
    margin = jnp.minimum(source_of - 1, reach - sink)
    moved = jax.random.randint(jax.random.fold_in(own_key, 1), (couples,), 0, 1 << 20) % (margin + 1)
    tallies = tallies.at[1:1 + 2 * couples:2].set(source_of - moved).at[2:2 + 2 * couples:2].set(sink + moved)
    return tallies[jax.random.permutation(jax.random.fold_in(own_key, 2), count)]


def normal_values(stream_key, shape, spread, limit, pieces=(), kind=jnp.bfloat16):
    level = block_scale(stream_key, shape, pieces, -0.22, 0.18) if pieces else 1.0
    array = jax.random.normal(stream_key, shape, jnp.float32) * spread * level
    return jnp.minimum(jnp.maximum(array, -limit), limit).astype(kind)


def setup_inputs(seed: int = 0) -> dict:
    arg_keys = jax.random.split(jax.random.key(seed), 16)
    return {
        "features": normal_values(arg_keys[0], (N_GROUP * SIDE, N_PEER * TPD * SIDE, C), 1.0, 6.0, ((0, 8), (1, 4)), jnp.float32),
        "image_of_row": jnp.searchsorted(jnp.cumsum(ragged(arg_keys[1], IMAGES, N_GROUP, 4, 1)), jnp.arange(N_GROUP), side="right").astype(jnp.int32),
        "llm_peer": draw_llm_peer(jax.random.fold_in(arg_keys[15], 71), 0),
        "token_grads": normal_values(arg_keys[3], (N_GROUP * N_PEER * CAP, POOLED * POOLED, C), 1.0, 6.0, ((0, 32),), jnp.float32),
        "dw_weight": normal_values(arg_keys[4], (49, C), 49 ** -0.5, 0.875, (), jnp.float32),
        "dw_bias": normal_values(arg_keys[5], (C,), 0.5, 3.0, (), jnp.float32),
        "ln_gain": jnp.clip(1.0 + 0.18 * jax.random.normal(arg_keys[6], (C,), jnp.float32), 0.1, 1.9),
        "ln_bias": normal_values(arg_keys[7], (C,), 0.5, 3.0, (), jnp.float32),
        "w_in": normal_values(arg_keys[8], (C, HID), C ** -0.5, 0.3125),
        "b_in": normal_values(arg_keys[9], (HID,), 0.5, 3.0, (), jnp.float32),
        "w_out": normal_values(arg_keys[10], (HID, C), HID ** -0.5, 0.15625),
        "b_out": normal_values(arg_keys[11], (C,), 0.5, 3.0, (), jnp.float32),
        "layer_scale": jnp.clip(jnp.exp(jax.random.uniform(arg_keys[12], (C,), jnp.float32, math.log(0.3), math.log(1.0))), 0.3, 1.0),
        "comp_weight": normal_values(arg_keys[13], (9, C, C), (9 * C) ** -0.5, 0.109375),
        "comp_bias": normal_values(arg_keys[14], (C,), 0.5, 3.0, (), jnp.float32),
    }


def encode(tile_data, params):
    dw_weight, dw_bias, ln_gain, ln_bias, w_in, b_in, w_out, b_out, layer_scale = params
    tile_side = tile_data.shape[1]
    channels = tile_data.shape[3]
    padded = jnp.pad(tile_data, ((0, 0), (3, 3), (3, 3), (0, 0)))
    spatial = jnp.zeros_like(tile_data) + dw_bias
    for offset in range(49):
        row_off = offset // 7
        col_off = offset % 7
        spatial = spatial + padded[:, row_off:row_off + tile_side, col_off:col_off + tile_side, :] * dw_weight[offset]
    average = lax.optimization_barrier(jnp.mean(spatial, axis=-1, keepdims=True))
    centered = spatial - average
    variance = lax.optimization_barrier(jnp.mean(centered * centered, axis=-1, keepdims=True))
    normed = centered * lax.rsqrt(variance + 1e-06) * ln_gain + ln_bias
    flattened = normed.reshape(-1, channels).astype(jnp.bfloat16)
    hidden = jax.nn.gelu(jnp.dot(flattened, w_in, preferred_element_type=jnp.float32) + b_in, approximate=False)
    branch = jnp.dot(hidden.astype(jnp.bfloat16), w_out, preferred_element_type=jnp.float32) + b_out
    return tile_data + layer_scale * branch.reshape(tile_data.shape)

def pool_tiles(tile_data):
    tile_count, tile_side, other_side, channels = tile_data.shape
    return tile_data.reshape(tile_count, tile_side // 2, 2, other_side // 2, 2, channels).mean(axis=(2, 4))

def spread_tiles(grad_data):
    return jnp.repeat(jnp.repeat(grad_data, 2, axis=1), 2, axis=2) * 0.25

def compress_conv(padded, kernel):
    out_rows = padded.shape[-3] - 2
    out_cols = padded.shape[-2] - 2
    leading = padded.shape[:-3]
    summed = jnp.zeros((1, kernel.shape[2]), jnp.float32)
    for offset in range(9):
        row_off = offset // 3
        col_off = offset % 3
        window = padded[..., row_off:row_off + out_rows, col_off:col_off + out_cols, :]
        window = window.reshape(-1, padded.shape[-1]).astype(jnp.bfloat16)
        summed = summed + jnp.dot(window, kernel[offset], preferred_element_type=jnp.float32)
    return summed.reshape(leading + (out_rows, out_cols, kernel.shape[2]))

def rim_pad(pool_grid, keep_up, keep_down):
    empty = jnp.zeros_like(pool_grid[:1, 0])
    above = jnp.concatenate([empty, pool_grid[:-1, -1]], axis=0) * keep_up[:, None, None]
    below = jnp.concatenate([pool_grid[1:, 0], empty], axis=0) * keep_down[:, None, None]
    stacked = jnp.concatenate([above[:, None], pool_grid, below[:, None]], axis=1)
    return jnp.pad(stacked, ((0, 0), (0, 0), (1, 1), (0, 0)))

def reference(features, image_of_row, llm_peer, token_grads, dw_weight, dw_bias, ln_gain, ln_bias, w_in, b_in, w_out, b_out, layer_scale, comp_weight, comp_bias):
    params = (dw_weight, dw_bias, ln_gain, ln_bias, w_in, b_in, w_out, b_out, layer_scale)
    groups = N_GROUP
    peer_count = N_PEER
    per_row = peer_count * TPD
    channels = features.shape[2]
    tile_groups = features.reshape(groups, SIDE, per_row, SIDE, channels).transpose(0, 2, 1, 3, 4)

    def run_block(tile_data):
        return encode(tile_data, params)
    encoded = lax.map(run_block, tile_groups)
    pooled = pool_tiles(encoded.reshape(-1, SIDE, SIDE, channels))
    pooled = pooled.reshape(groups, per_row, POOLED, POOLED, channels)
    pool_grid = pooled.transpose(0, 2, 1, 3, 4).reshape(groups, POOLED, per_row * POOLED, channels)
    same_image = (image_of_row[1:] == image_of_row[:-1]).astype(jnp.float32)
    zero_one = jnp.zeros((1,), jnp.float32)
    keep_up = jnp.concatenate([zero_one, same_image])
    keep_down = jnp.concatenate([same_image, zero_one])
    compressed = compress_conv(rim_pad(pool_grid, keep_up, keep_down), comp_weight) + comp_bias
    comp_tiles = compressed.reshape(groups, POOLED, peer_count, TPD, POOLED, channels)
    comp_tiles = comp_tiles.transpose(0, 2, 3, 1, 4, 5).reshape(groups, peer_count, TPD, POOLED * POOLED, channels)
    route_hot = (llm_peer.reshape(groups, peer_count, TPD)[..., None] == jnp.arange(peer_count, dtype=jnp.int32)).astype(jnp.float32)
    sends = lax.optimization_barrier(jnp.sum(route_hot, axis=2))
    before = jnp.cumsum(sends, axis=1) - sends
    slot_hot = (before[..., None] == jnp.arange(CAP, dtype=jnp.int32).astype(jnp.float32)).astype(jnp.float32)
    full_hot = route_hot[..., None] * slot_hot[:, :, None]
    llm_tokens = jnp.einsum('gptds,gptxc->gdsxc', full_hot, comp_tiles, precision=lax.Precision.HIGHEST)
    llm_tokens = llm_tokens.reshape(groups * peer_count * CAP, POOLED * POOLED, channels)
    incoming = token_grads.reshape(groups, peer_count, CAP, POOLED * POOLED, channels)
    grad_tiles = jnp.einsum('gptds,gdsxc->gptxc', full_hot, incoming, precision=lax.Precision.HIGHEST)
    grad_grid = grad_tiles.reshape(groups, peer_count, TPD, POOLED, POOLED, channels)
    grad_grid = grad_grid.transpose(0, 3, 1, 2, 4, 5).reshape(groups, POOLED, per_row * POOLED, channels)
    flipped = jnp.transpose(comp_weight[::-1], (0, 2, 1))
    grad_pooled = compress_conv(rim_pad(grad_grid, keep_up, keep_down), flipped)
    grad_pooled = grad_pooled.reshape(groups, POOLED, per_row, POOLED, channels).transpose(0, 2, 1, 3, 4)
    grad_encoded = spread_tiles(grad_pooled.reshape(-1, POOLED, POOLED, channels))
    grad_encoded = grad_encoded.reshape(groups, per_row, SIDE, SIDE, channels)

    def pull_back(pair):
        tile_data, grad_data = pair
        pullback = jax.vjp(run_block, tile_data)[1]
        return pullback(grad_data)[0]
    grad_input = lax.map(pull_back, (tile_groups, grad_encoded))
    feature_grads = grad_input.transpose(0, 2, 1, 3, 4).reshape(groups * SIDE, per_row * SIDE, channels)
    return (llm_tokens, feature_grads)
```

```python
import functools
import math
import types

import jax
import jax.numpy as jnp
from jax import lax
from jax.experimental import pallas as pl
from jax.experimental.pallas import tpu as pltpu
from jax.sharding import PartitionSpec as P

MESH = pl.DeviceIdType.MESH
LANES = 128
PAD = 8
BLOCK = 256
WIDE = 16


def nt_dot(a, b):
    return lax.dot_general(a, b, (((1,), (1,)), ((), ())), preferred_element_type=jnp.float32)


def depthwise(src, weight, chunk, taps, side, flip):
    half = side // 2
    reach = taps // 2
    outs = []
    for parity in range(2):
        total = None
        for b in range(taps):
            rows = src[chunk, :, pl.ds(PAD - reach + parity + b, half, stride=2), :]
            for a in range(taps):
                k = (taps - 1 - a) * taps + taps - 1 - b if flip else a * taps + b
                term = rows[a : a + side] * weight[chunk, k : k + 1, :]
                total = term if total is None else total + term
        outs.append(total)
    return outs


def kernel(groups, peers, taps, names, *refs):
    r = types.SimpleNamespace(**dict(zip(names, refs)))
    g = lax.axis_index("group")
    me = lax.axis_index("peer")
    side = r.x_hbm.shape[0]
    channels = r.x_hbm.shape[2]
    half = side // 2
    cells = half * half
    chunks = channels // LANES
    reach = taps // 2
    hid = r.win.shape[1]
    slots = r.tg.shape[0]
    pairs = peers // 2
    core = lax.rem(me, 2)
    partner = me + 1 - 2 * core
    small = (r.dwb, r.gain, r.lnb, r.bout, r.scale, r.cb)
    inner = slice(PAD, PAD + half)

    def vector(ref, lane=slice(None)):
        return ref[lane].reshape(1, -1)

    def seat(k, which):
        return lax.rem(lax.div(me, 2) + k, pairs) * 2 + which

    beyond = {-1: g > 0, 1: g < groups - 1}

    for buf in (r.grow, r.gcorn_in, r.arow, r.acorn):
        buf[...] = jnp.zeros_like(buf)
    barrier = pltpu.get_barrier_semaphore()

    def greet(row, who):
        pl.semaphore_signal(barrier, inc=1, device_id={"group": row, "peer": who}, device_id_type=MESH)

    for k in range(1, peers):
        greet(g, lax.rem(me + k, peers))
    for dr in (-1, 1):

        @pl.when(beyond[dr])
        def _():
            for k in range(pairs):
                greet(g + dr, seat(k, core))

    copies = {}

    def fetch(name, src, dst):
        copy = pltpu.make_async_copy(src, dst, r.in_sems.at[len(copies)])
        copy.start()
        copies[name] = copy

    fetch("owner", r.owner_hbm, r.owner_ref)
    fetch("tg", r.tg_hbm, r.tg)
    for c in range(chunks):
        lane = slice(c * LANES, (c + 1) * LANES)
        fetch(("w", c), r.dww_hbm.at[:, lane], r.dww.at[c])
        fetch(("x", c), r.x_hbm.at[:, :, lane], r.xpad.at[c, reach : reach + side, PAD : PAD + side, :])
    for i, src in enumerate((r.dwb_hbm, r.gain_hbm, r.lnb_hbm, r.bout_hbm, r.scale_hbm, r.cb_hbm)):
        fetch(("s", i), src, small[i])
    fetch("image", r.image_hbm, r.image_ref)
    fetch("bin", r.bin_hbm, r.bin_)
    fetch("win", r.win_hbm, r.win)
    fetch("wout", r.wout_hbm, r.wout)
    fetch("cw", r.cw_hbm, r.cw)

    def clear(buf):
        width = buf.shape[2]
        for c in range(chunks):
            buf[c, :reach] = jnp.zeros((reach, width, LANES), jnp.float32)
            buf[c, reach + side :] = jnp.zeros((reach, width, LANES), jnp.float32)
            buf[c, reach : reach + side, :PAD] = jnp.zeros((side, PAD, LANES), jnp.float32)
            buf[c, reach : reach + side, PAD + side :] = jnp.zeros((side, PAD, LANES), jnp.float32)

    clear(r.xpad)
    clear(r.gpad)
    r.grid_p[...] = jnp.zeros_like(r.grid_p)

    def move(src, dst, sems, index, where, row=None):
        send, recv = sems
        return pltpu.make_async_remote_copy(
            src_ref=src,
            dst_ref=dst,
            send_sem=send.at[index],
            recv_sem=recv.at[index],
            device_id={"group": g if row is None else row, "peer": where},
            device_id_type=MESH,
        )

    copies["owner"].wait()
    r.table[me] = jnp.full((8, LANES), r.owner_ref[0, 0], jnp.int32)
    along = (g > 0).astype(jnp.int32) + (g < groups - 1).astype(jnp.int32)
    pl.semaphore_wait(barrier, peers - 1 + pairs * along)

    tab_sems = (r.tab_send, r.tab_recv)
    table_moves = [
        move(r.table.at[me], r.table.at[me], tab_sems, k - 1, lax.rem(me + k, peers)) for k in range(1, peers)
    ]
    for m in table_moves:
        m.start()
    copies["tg"].wait()
    near_move = move(r.tg, r.ntg, (r.near_send, r.near_recv), 0, partner)
    near_move.start()

    def forward_conv(c):
        outs = depthwise(r.xpad, r.dww, c, taps, side, False)
        bias = vector(small[0], slice(c * LANES, (c + 1) * LANES))
        for parity in range(2):
            part = (outs[parity] + bias).reshape(half, 2, half, LANES)
            for row in range(2):
                r.sp[c, row * 2 + parity] = part[:, row].reshape(cells, LANES)

    copies[("s", 0)].wait()
    for c in range(chunks):
        copies[("w", c)].wait()
        copies[("x", c)].wait()
        forward_conv(c)
    for m in table_moves:
        m.wait()
    near_move.wait()

    def masks_of(who, device):
        inside = jnp.logical_and(who >= 0, who < peers)
        at = jnp.clip(who, 0, peers - 1)
        mine = jnp.logical_and(r.table[at] == device, inside)
        before = jnp.zeros((8, LANES), jnp.int32)
        for p in range(peers):
            earlier = (p < at).astype(jnp.int32)
            before = before + jnp.where(r.table[p] == device, earlier, 0)
        return [jnp.logical_and(mine, before == s).astype(jnp.float32) for s in range(slots)]

    def wide(mask):
        return jnp.concatenate([mask] * chunks, axis=1)

    def held(who):
        pairs_of = []
        for ref, device in ((r.tg, me), (r.ntg, partner)):
            for s, mask in enumerate(masks_of(who, device)):
                pairs_of.append((ref, s, wide(mask)))
        return pairs_of

    def total_of(terms):
        return functools.reduce(jnp.add, terms)

    for k in range(pairs):
        home = seat(k, core)
        r.gmain[k] = total_of([ref[s] * mask for ref, s, mask in held(home)])
        left = total_of([ref[s, :, half - 1, :] * mask for ref, s, mask in held(home - 1)])
        right = total_of([ref[s, :, 0, :] * mask for ref, s, mask in held(home + 1)])
        r.gcols[k, 0] = left
        r.gcols[k, 1] = right
        for d, at in ((0, 0), (1, half - 1)):
            r.gcorn[k, d, 0:1, :] = left[at : at + 1]
            r.gcorn[k, d, 1:2, :] = right[at : at + 1]

    row_sems = (r.row_send, r.row_recv)
    cor_sems = (r.cor_send, r.cor_recv)

    def row_moves(src_row, src_corner, dst_row, dst_corner, sems_r, sems_c):
        moves = {}
        for d, dr in ((0, -1), (1, 1)):
            for k in range(pairs):
                moves[d, k] = (
                    move(src_row(d, k), dst_row(d, k), sems_r, d * pairs + k, seat(k, core), g + dr),
                    move(src_corner(d, k), dst_corner(d, k), sems_c, d * pairs + k, seat(k, core), g + dr),
                )
        return moves

    def start_rows(moves):
        for d, dr in ((0, -1), (1, 1)):

            @pl.when(beyond[dr])
            def _():
                for k in reversed(range(pairs)):
                    for m in moves[d, k]:
                        m.start()

    def sent_rows(moves):
        for d, dr in ((0, -1), (1, 1)):

            @pl.when(beyond[dr])
            def _():
                for k in range(pairs):
                    for m in moves[d, k]:
                        m.wait_send()

    def received_rows(moves):
        for d, dr in ((0, -1), (1, 1)):

            @pl.when(beyond[-dr])
            def _():
                for k in range(pairs):
                    for m in moves[d, k]:
                        m.wait_recv()

    g_rows = row_moves(
        lambda d, k: r.gmain.at[k, 0 if d == 0 else half - 1],
        lambda d, k: r.gcorn.at[k, d],
        lambda d, k: r.grow.at[d, k],
        lambda d, k: r.gcorn_in.at[d, k],
        row_sems,
        cor_sems,
    )
    start_rows(g_rows)
    far_sems = (r.far_send, r.far_recv)
    g_far = []
    for k in range(1, pairs):
        g_far.append(move(r.gcols.at[k], r.rcols.at[k - 1], far_sems, 2 * k - 2, seat(k, core)))
        g_far.append(move(r.gmain.at[k], r.rmain.at[k - 1], far_sems, 2 * k - 1, seat(k, core)))
    for m in g_far:
        m.start()

    for i in range(1, 6):
        copies[("s", i)].wait()
    for q in range(4):
        parts = [r.sp[c, q] for c in range(chunks)]
        mean = jnp.sum(functools.reduce(jnp.add, parts), axis=1, keepdims=True) / channels
        parts = [part - mean for part in parts]
        square = functools.reduce(jnp.add, [part * part for part in parts])
        inv = lax.rsqrt(jnp.sum(square, axis=1, keepdims=True) / channels + 1e-06)
        r.rstd[q] = jnp.broadcast_to(inv, (cells, LANES))
        for c in range(chunks):
            lane = slice(c * LANES, (c + 1) * LANES)
            hat = parts[c] * inv
            r.sp[c, q] = hat
            r.nb[q * cells : (q + 1) * cells, lane] = (
                hat * vector(small[1], lane) + vector(small[2], lane)
            ).astype(jnp.bfloat16)

    copies["bin"].wait()
    copies["image"].wait()
    copies["win"].wait()
    for n in range(hid // BLOCK):
        lane = slice(n * BLOCK, (n + 1) * BLOCK)
        pre_all = jnp.dot(r.nb[...], r.win[:, lane], preferred_element_type=jnp.float32)
        bias = vector(r.bin_, lane)
        pooled = None
        for q in range(4):
            pre = pre_all[q * cells : (q + 1) * cells] + bias
            cdf = 0.5 + 0.5 * lax.erf(pre * math.sqrt(0.5))
            pdf = jnp.exp(pre * pre * -0.5) * (1.0 / math.sqrt(2.0 * math.pi))
            r.dg[q * cells : (q + 1) * cells, lane] = cdf + pre * pdf
            value = pre * cdf
            pooled = value if pooled is None else pooled + value
        r.hb[:, lane] = (pooled * 0.25).astype(jnp.bfloat16)
    copies["wout"].wait()
    branch = jnp.dot(r.hb[...], r.wout[...], preferred_element_type=jnp.float32)
    for c in range(chunks):
        lane = slice(c * LANES, (c + 1) * LANES)
        total = None
        for row in range(2):
            for parity in range(2):
                part = r.xpad[c, reach : reach + side, pl.ds(PAD + parity, half, stride=2), :]
                part = part.reshape(half, 2, half, LANES)[:, row]
                total = part if total is None else total + part
        mixed = vector(small[4], lane) * (branch[:, lane] + vector(small[3], lane))
        r.grid_p[2 : half + 2, inner, lane] = total * 0.25 + mixed.reshape(half, half, LANES)

    copies["cw"].wait()
    rim = half + 2
    comp = None
    for a in range(3):
        for b in range(3):
            part = r.grid_p[a : a + rim, PAD - 2 + b : PAD - 2 + b + WIDE, :]
            part = part.reshape(rim * WIDE, channels).astype(jnp.bfloat16)
            part = jnp.dot(part, r.cw[a * 3 + b], preferred_element_type=jnp.float32)
            comp = part if comp is None else comp + part
    comp = comp.reshape(rim, WIDE, channels)
    r.amain[me] = comp[1 : half + 1, 1 : half + 1]
    for d, at in ((0, 0), (1, half + 1)):
        r.acols[me, d] = comp[1 : half + 1, at]
        r.erow[d] = comp[at, 1 : half + 1]
        r.ecorn[d, 0:1, :] = comp[at, 0:1]
        r.ecorn[d, 1:2, :] = comp[at, half + 1 : half + 2]

    trow_sems = (r.trow_send, r.trow_recv)
    tcor_sems = (r.tcor_send, r.tcor_recv)
    t_rows = row_moves(
        lambda d, k: r.erow.at[d],
        lambda d, k: r.ecorn.at[d],
        lambda d, k: r.arow.at[d, me],
        lambda d, k: r.acorn.at[d, me],
        trow_sems,
        tcor_sems,
    )
    start_rows(t_rows)
    tok_sems = (r.tok_send, r.tok_recv)
    t_far = []
    for k in range(1, pairs):
        t_far.append(move(r.acols.at[me], r.acols.at[me], tok_sems, 2 * k, seat(k, core)))
        t_far.append(move(r.amain.at[me], r.amain.at[me], tok_sems, 2 * k + 1, seat(k, core)))
    t_near = [
        move(r.acols.at[me], r.acols.at[me], tok_sems, 0, partner),
        move(r.amain.at[me], r.amain.at[me], tok_sems, 1, partner),
    ]
    for m in t_far + t_near:
        m.start()

    image = r.image_ref[g]
    keep = {}
    for d, near in ((1, jnp.maximum(g - 1, 0)), (0, jnp.minimum(g + 1, groups - 1))):
        there = (g > 0) if d == 1 else (g < groups - 1)
        keep[d] = (r.image_ref[near] == image).astype(jnp.float32) * there.astype(jnp.float32)

    received_rows(g_rows)
    for m in g_far:
        m.wait_recv()
    def far(own, other):
        return total_of([own] + [other(k) for k in range(pairs - 1)])
    r.grid_g[1 : half + 1, inner, :] = far(r.gmain[0], lambda k: r.rmain[k])
    r.grid_g[1 : half + 1, PAD - 1, :] = far(r.gcols[0, 0], lambda k: r.rcols[k, 0])
    r.grid_g[1 : half + 1, PAD + half, :] = far(r.gcols[0, 1], lambda k: r.rcols[k, 1])
    for d, row in ((1, 0), (0, half + 1)):
        r.grid_g[row, inner, :] = total_of([r.grow[d, k] for k in range(pairs)]) * keep[d]
        corner = total_of([r.gcorn_in[d, k] for k in range(pairs)]) * keep[d]
        r.grid_g[row, PAD - 1 : PAD, :] = corner[0:1]
        r.grid_g[row, PAD + half : PAD + half + 1, :] = corner[1:2]

    grads = None
    for a in range(3):
        for b in range(3):
            part = r.grid_g[a : a + half, PAD - 1 + b : PAD - 1 + b + half, :]
            part = part.reshape(cells, channels).astype(jnp.bfloat16)
            part = nt_dot(part, r.cw[(2 - a) * 3 + 2 - b])
            grads = part if grads is None else grads + part
    grads = grads * 0.25
    for c in range(chunks):
        lane = slice(c * LANES, (c + 1) * LANES)
        r.gq[c] = grads[:, lane].reshape(half, half, LANES)
    scaled = (grads * vector(r.scale)).astype(jnp.bfloat16)

    for n in range(hid // BLOCK):
        lane = slice(n * BLOCK, (n + 1) * BLOCK)
        dh = nt_dot(scaled, r.wout[lane, :])
        for q in range(4):
            rows = slice(q * cells, (q + 1) * cells)
            r.dpb[rows, lane] = (dh * r.dg[rows, lane]).astype(jnp.bfloat16)
    dn_all = nt_dot(r.dpb[...], r.win[...])
    for q in range(4):
        dn = dn_all[q * cells : (q + 1) * cells] * vector(r.gain)
        parts = [dn[:, c * LANES : (c + 1) * LANES] for c in range(chunks)]
        first = jnp.sum(functools.reduce(jnp.add, parts), axis=1, keepdims=True) / channels
        cross = functools.reduce(jnp.add, [parts[c] * r.sp[c, q] for c in range(chunks)])
        second = jnp.sum(cross, axis=1, keepdims=True) / channels
        for c in range(chunks):
            back = r.rstd[q] * (parts[c] - first - r.sp[c, q] * second)
            back = back.reshape(half, half, LANES)
            for i in range(half):
                r.gpad[c, reach + 2 * i + q // 2, pl.ds(PAD + q % 2, half, stride=2), :] = back[i]

    def backward_conv(c):
        outs = depthwise(r.gpad, r.dww, c, taps, side, True)
        direct = jnp.broadcast_to(r.gq[c][:, None], (half, 2, half, LANES)).reshape(side, half, LANES)
        for parity in range(2):
            value = outs[parity] + direct
            for i in range(side):
                r.obuf[c, i, pl.ds(parity, half, stride=2), :] = value[i]

    for c in range(chunks - 1):
        backward_conv(c)

    received_rows(t_rows)
    for m in t_far:
        m.wait_recv()
    pass_sems = (r.pass_send, r.pass_recv)
    passed = []
    for k in range(1, pairs):
        who = seat(pairs - k, core)
        passed.append(move(r.acols.at[who], r.acols.at[who], pass_sems, 2 * k - 2, partner))
        passed.append(move(r.amain.at[who], r.amain.at[who], pass_sems, 2 * k - 1, partner))
    for m in passed:
        m.start()
    prow_sems = (r.prow_send, r.prow_recv)
    pcor_sems = (r.pcor_send, r.pcor_recv)
    passed_rows = {}
    for d, dr in ((0, -1), (1, 1)):
        for k in range(pairs):
            who = seat(k, core)
            passed_rows[d, k] = (
                move(r.arow.at[d, who], r.arow.at[d, who], prow_sems, d * pairs + k, partner),
                move(r.acorn.at[d, who], r.acorn.at[d, who], pcor_sems, d * pairs + k, partner),
            )
        @pl.when(beyond[-dr])
        def _():
            for k in range(pairs):
                for m in passed_rows[d, k]:
                    m.start()

    backward_conv(chunks - 1)

    for m in t_near + passed:
        m.wait()
    for m in t_far + g_far:
        m.wait_send()
    sent_rows(g_rows)
    sent_rows(t_rows)
    for d, dr in ((0, -1), (1, 1)):

        @pl.when(beyond[-dr])
        def _():
            for k in range(pairs):
                for m in passed_rows[d, k]:
                    m.wait()

    chosen = [[wide(mask) for mask in masks_of(p, me)] for p in range(peers)]
    bias = vector(r.cb)
    for s in range(slots):
        total = None
        west = jnp.zeros((half, channels), jnp.float32)
        east = jnp.zeros((half, channels), jnp.float32)
        line = {d: jnp.zeros((half, channels), jnp.float32) for d in range(2)}
        tips = {d: [jnp.zeros((1, channels), jnp.float32) for _ in range(2)] for d in range(2)}
        for p in range(peers):
            mask = chosen[p][s]
            part = (r.amain[p] + bias) * mask
            total = part if total is None else total + part
            if p > 0:
                west = west + r.acols[p - 1, 1] * mask
            if p < peers - 1:
                east = east + r.acols[p + 1, 0] * mask
            for d in range(2):
                line[d] = line[d] + r.arow[d, p] * mask
                if p > 0:
                    tips[d][0] = tips[d][0] + r.acorn[d, p - 1, 1:2, :] * mask[:1]
                if p < peers - 1:
                    tips[d][1] = tips[d][1] + r.acorn[d, p + 1, 0:1, :] * mask[:1]
        r.tokout[s] = total
        r.tokout[s, :, 0, :] += west
        r.tokout[s, :, half - 1, :] += east
        for d, row in ((1, 0), (0, half - 1)):
            r.tokout[s, row] += line[d] * keep[d]
            r.tokout[s, row, 0:1, :] += tips[d][0] * keep[d]
            r.tokout[s, row, half - 1 : half, :] += tips[d][1] * keep[d]


def tail(obuf, tokout, tok_hbm, dx_hbm, sems):
    chunks = obuf.shape[0]
    copies = [pltpu.make_async_copy(tokout, tok_hbm, sems.at[chunks])]
    for c in range(chunks):
        copies.append(
            pltpu.make_async_copy(obuf.at[c], dx_hbm.at[:, :, c * LANES : (c + 1) * LANES], sems.at[c])
        )
    for copy in copies:
        copy.start()
    for copy in copies:
        copy.wait()


def solution(mesh):
    groups, peers = mesh.shape["group"], mesh.shape["peer"]

    def on_device(
        features, image_of_row, llm_peer, token_grads, dw_weight, dw_bias, ln_gain, ln_bias,
        w_in, b_in, w_out, b_out, layer_scale, comp_weight, comp_bias,
    ):
        side, width, channels = features.shape
        slots = token_grads.shape[0]
        hid = w_in.shape[1]
        taps = math.isqrt(dw_weight.shape[0])
        half = side // 2
        cells = half * half
        chunks = channels // LANES
        assert width == side and llm_peer.shape == (1, 1)
        f32, bf16 = jnp.float32, jnp.bfloat16
        padded = (chunks, side + 2 * (taps // 2), side + 2 * PAD, LANES)
        block = (half, half, channels)
        strip = (half, channels)
        tip = (2, channels)
        hbm = pl.BlockSpec(memory_space=pltpu.HBM)
        pairs = peers // 2
        assert peers == 2 * pairs and pairs > 1
        vmem = pl.BlockSpec(memory_space=pltpu.VMEM)

        def dma(count):
            return pltpu.SemaphoreType.DMA((count,))

        def buf(*shape, kind=f32):
            return pltpu.VMEM(shape, kind)

        inputs = (
            "image_hbm", "owner_hbm", "x_hbm", "tg_hbm", "dww_hbm", "dwb_hbm", "gain_hbm", "lnb_hbm",
            "win_hbm", "bin_hbm", "wout_hbm", "bout_hbm", "scale_hbm", "cw_hbm", "cb_hbm",
        )
        held = {
            "obuf": buf(chunks, side, side, LANES),
            "tokout": buf(slots, *block),
        }
        scratch = {
            "xpad": buf(*padded),
            "gpad": buf(*padded),
            "dww": buf(chunks, taps * taps, LANES),
            "gq": buf(chunks, half, half, LANES),
            "dwb": buf(channels),
            "gain": buf(channels),
            "lnb": buf(channels),
            "bout": buf(channels),
            "scale": buf(channels),
            "cb": buf(channels),
            "bin_": buf(hid),
            "win": buf(*w_in.shape, kind=bf16),
            "wout": buf(*w_out.shape, kind=bf16),
            "cw": buf(*comp_weight.shape, kind=bf16),
            "tg": buf(slots, *block),
            "ntg": buf(slots, *block),
            "sp": buf(chunks, 4, cells, LANES),
            "rstd": buf(4, cells, LANES),
            "nb": buf(4 * cells, channels, kind=bf16),
            "dg": buf(4 * cells, hid),
            "hb": buf(cells, hid, kind=bf16),
            "dpb": buf(4 * cells, hid, kind=bf16),
            "table": buf(peers, 8, LANES, kind=jnp.int32),
            "gmain": buf(pairs, *block),
            "gcols": buf(pairs, 2, *strip),
            "gcorn": buf(pairs, 2, *tip),
            "rmain": buf(pairs - 1, *block),
            "rcols": buf(pairs - 1, 2, *strip),
            "grow": buf(2, pairs, *strip),
            "gcorn_in": buf(2, pairs, *tip),
            "grid_g": buf(half + 2, half + 2 * PAD, channels),
            "grid_p": buf(half + 4, half + 2 * PAD, channels),
            "erow": buf(2, *strip),
            "ecorn": buf(2, *tip),
            "amain": buf(peers, *block),
            "acols": buf(peers, 2, *strip),
            "arow": buf(2, peers, *strip),
            "acorn": buf(2, peers, *tip),
            "image_ref": pltpu.SMEM(image_of_row.shape, jnp.int32),
            "owner_ref": pltpu.SMEM((1, 1), jnp.int32),
            "in_sems": dma(2 * chunks + 13),
        }
        for name, count in (
            ("tab", peers - 1), ("near", 1), ("row", 2 * pairs), ("cor", 2 * pairs), ("far", 2 * pairs - 2),
            ("trow", 2 * pairs), ("tcor", 2 * pairs), ("tok", 2 * pairs), ("pass", 2 * pairs - 2),
            ("prow", 2 * pairs), ("pcor", 2 * pairs),
        ):
            scratch[name + "_send"] = dma(count)
            scratch[name + "_recv"] = dma(count)
        names = inputs + tuple(held) + tuple(scratch)
        state = pl.pallas_call(
            functools.partial(kernel, groups, peers, taps, names),
            out_shape=tuple(held.values()),
            in_specs=[hbm] * len(inputs),
            out_specs=(vmem,) * len(held),
            scratch_shapes=list(scratch.values()),
            compiler_params=pltpu.CompilerParams(collective_id=0, has_side_effects=True),
        )(
            image_of_row,
            llm_peer,
            features,
            token_grads.reshape((slots,) + block),
            dw_weight,
            dw_bias,
            ln_gain,
            ln_bias,
            w_in,
            b_in,
            w_out,
            b_out,
            layer_scale,
            comp_weight,
            comp_bias,
        )
        tokens, grads = pl.pallas_call(
            tail,
            out_shape=(
                jax.ShapeDtypeStruct((slots,) + block, f32),
                jax.ShapeDtypeStruct(features.shape, f32),
            ),
            in_specs=[vmem] * len(held),
            out_specs=(hbm, hbm),
            scratch_shapes=[dma(chunks + 1)],
            compiler_params=pltpu.CompilerParams(vmem_limit_bytes=16 << 20),
        )(*state)
        return tokens.reshape(slots, cells, channels), grads

    placed = [P()] * 15
    placed[0] = P("group", "peer", None)
    placed[2] = P(("group", "peer"), None)
    placed[3] = P(("group", "peer"), None, None)
    return jax.shard_map(
        on_device,
        mesh=mesh,
        in_specs=tuple(placed),
        out_specs=(P(("group", "peer"), None, None), P("group", "peer", None)),
        check_vma=False,
    )
```

```python
import functools
import math
import types

import jax
import jax.numpy as jnp
from jax import lax
from jax.experimental import pallas as pl
from jax.experimental.pallas import tpu as pltpu
from jax.sharding import PartitionSpec as P

MESH = pl.DeviceIdType.MESH
LANES = 128
PAD = 8
BLOCK = 256
WIDE = 16
TABLE, NEAR, GROWS, GFAR, TROWS, TFAR, TNEAR, PASS, PROWS = 0, 1, 2, 4, 5, 7, 8, 9, 10
SENT_BY = (0, 0, 1, 2, 0, 1, 2, 0, 0, 0, 3, 4)


def nt_dot(a, b):
    return lax.dot_general(a, b, (((1,), (1,)), ((), ())), preferred_element_type=jnp.float32)


def depthwise(src, weight, chunk, taps, side, flip):
    half = side // 2
    reach = taps // 2
    outs = []
    for parity in range(2):
        total = None
        for b in range(taps):
            rows = src[chunk, :, pl.ds(PAD - reach + parity + b, half, stride=2), :]
            for a in range(taps):
                k = (taps - 1 - a) * taps + taps - 1 - b if flip else a * taps + b
                term = rows[a : a + side] * weight[chunk, k : k + 1, :]
                total = term if total is None else total + term
        outs.append(total)
    return outs


def kernel(groups, peers, taps, names, *refs):
    r = types.SimpleNamespace(**dict(zip(names, refs)))
    g = lax.axis_index("group")
    me = lax.axis_index("peer")
    side = r.x_hbm.shape[0]
    channels = r.x_hbm.shape[2]
    half = side // 2
    cells = half * half
    chunks = channels // LANES
    reach = taps // 2
    hid = r.win.shape[1]
    slots = r.tg.shape[0]
    pairs = peers // 2
    core = lax.rem(me, 2)
    partner = me + 1 - 2 * core
    inner = slice(PAD, PAD + half)

    def vector(ref, lane=slice(None)):
        return ref[lane].reshape(1, -1)

    def seat(k, which):
        return lax.rem(lax.div(me, 2) + k, pairs) * 2 + which

    beyond = {-1: g > 0, 1: g < groups - 1}

    for buf in (r.grow, r.gcorn_in, r.arow, r.acorn):
        buf[...] = jnp.zeros_like(buf)
    barrier = pltpu.get_barrier_semaphore()

    def greet(row, who):
        pl.semaphore_signal(barrier, inc=1, device_id={"group": row, "peer": who}, device_id_type=MESH)

    for k in range(1, peers):
        greet(g, lax.rem(me + k, peers))
    for dr in (-1, 1):

        @pl.when(beyond[dr])
        def _():
            greet(g + dr, me)

    copies = {}

    def fetch(name, *moves):
        sem = r.in_sems.at[len(copies)]
        copies[name] = [pltpu.make_async_copy(src, dst, sem) for src, dst in moves]
        for copy in copies[name]:
            copy.start()

    def settle(sem, elements):
        span = r.span.at[pl.ds(0, elements // LANES)]
        pltpu.make_async_copy(span, span, sem).wait()

    def fetched(name):
        if len(copies[name]) == 1:
            copies[name][0].wait()
        else:
            elements = sum(math.prod(copy.dst_ref.shape) for copy in copies[name])
            settle(r.in_sems.at[list(copies).index(name)], elements)

    fetch("owner", (r.owner_hbm, r.owner_ref))
    fetch("tg", (r.tg_hbm, r.tg))
    fetch(
        "small",
        (r.dwb_hbm, r.dwb),
        (r.gain_hbm, r.gain),
        (r.lnb_hbm, r.lnb),
        (r.bout_hbm, r.bout),
        (r.scale_hbm, r.scale),
        (r.cb_hbm, r.cb),
        (r.bin_hbm, r.bin_),
    )
    by_lane = []
    for c in range(chunks):
        lane = slice(c * LANES, (c + 1) * LANES)
        by_lane.append((r.dww_hbm.at[:, lane], r.dww.at[c]))
        by_lane.append((r.x_hbm.at[:, :, lane], r.xpad.at[c, reach : reach + side, PAD : PAD + side, :]))
    fetch("x", *by_lane)
    fetch("image", (r.image_hbm, r.image_ref))
    fetch("win", (r.win_hbm, r.win))
    fetch("wout", (r.wout_hbm, r.wout))
    fetch("cw", (r.cw_hbm, r.cw))

    def clear(buf):
        width = buf.shape[2]
        for c in range(chunks):
            buf[c, :reach] = jnp.zeros((reach, width, LANES), jnp.float32)
            buf[c, reach + side :] = jnp.zeros((reach, width, LANES), jnp.float32)
            buf[c, reach : reach + side, :PAD] = jnp.zeros((side, PAD, LANES), jnp.float32)
            buf[c, reach : reach + side, PAD + side :] = jnp.zeros((side, PAD, LANES), jnp.float32)

    clear(r.xpad)
    clear(r.gpad)
    r.grid_p[...] = jnp.zeros_like(r.grid_p)

    def move(src, dst, group, where, row=None):
        return pltpu.make_async_remote_copy(
            src_ref=src,
            dst_ref=dst,
            send_sem=r.send.at[SENT_BY[group]],
            recv_sem=r.recv.at[group],
            device_id={"group": g if row is None else row, "peer": where},
            device_id_type=MESH,
        )

    fetched("owner")
    r.table[me] = jnp.full((8, LANES), r.owner_ref[0, 0], jnp.int32)
    along = (g > 0).astype(jnp.int32) + (g < groups - 1).astype(jnp.int32)
    pl.semaphore_wait(barrier, peers - 1 + along)

    table_moves = [
        move(r.table.at[me], r.table.at[me], TABLE, lax.rem(me + k, peers)) for k in range(1, peers)
    ]
    for m in table_moves:
        m.start()
    fetched("tg")
    near_move = move(r.tg, r.ntg, NEAR, partner)
    near_move.start()

    def forward_conv(c):
        outs = depthwise(r.xpad, r.dww, c, taps, side, False)
        bias = vector(r.dwb, slice(c * LANES, (c + 1) * LANES))
        for parity in range(2):
            part = (outs[parity] + bias).reshape(half, 2, half, LANES)
            for row in range(2):
                r.sp[c, row * 2 + parity] = part[:, row].reshape(cells, LANES)

    fetched("small")
    fetched("x")
    for c in range(chunks):
        forward_conv(c)
    tile = cells * channels
    edge = half * channels
    main = (pairs - 1) * (tile + 2 * edge)
    strips = pairs * (edge + 2 * channels)
    settle(r.recv.at[TABLE], (peers - 1) * 8 * LANES)
    settle(r.recv.at[NEAR], slots * tile)

    def masks_of(who, device):
        inside = jnp.logical_and(who >= 0, who < peers)
        at = jnp.clip(who, 0, peers - 1)
        mine = jnp.logical_and(r.table[at] == device, inside)
        before = jnp.zeros((8, LANES), jnp.int32)
        for p in range(peers):
            earlier = (p < at).astype(jnp.int32)
            before = before + jnp.where(r.table[p] == device, earlier, 0)
        return [jnp.logical_and(mine, before == s).astype(jnp.float32) for s in range(slots)]

    def wide(mask):
        return jnp.concatenate([mask] * chunks, axis=1)

    def held(who):
        pairs_of = []
        for ref, device in ((r.tg, me), (r.ntg, partner)):
            for s, mask in enumerate(masks_of(who, device)):
                pairs_of.append((ref, s, wide(mask)))
        return pairs_of

    def total_of(terms):
        return functools.reduce(jnp.add, terms)

    for k in range(pairs):
        home = seat(k, core)
        r.gmain[k] = total_of([ref[s] * mask for ref, s, mask in held(home)])
        left = total_of([ref[s, :, half - 1, :] * mask for ref, s, mask in held(home - 1)])
        right = total_of([ref[s, :, 0, :] * mask for ref, s, mask in held(home + 1)])
        r.gcols[k, 0] = left
        r.gcols[k, 1] = right
        for d, at in ((0, 0), (1, half - 1)):
            r.gcorn[k, d, 0:1, :] = left[at : at + 1]
            r.gcorn[k, d, 1:2, :] = right[at : at + 1]

    def row_moves(src_row, src_corner, dst_row, dst_corner, group, which):
        moves = {}
        for d, dr in ((0, -1), (1, 1)):
            for k in range(pairs):
                moves[d, k] = (
                    move(src_row(d, k), dst_row(d, k), group + d, seat(k, which), g + dr),
                    move(src_corner(d, k), dst_corner(d, k), group + d, seat(k, which), g + dr),
                )
        return moves

    def start_rows(moves):
        for d, dr in ((0, -1), (1, 1)):

            @pl.when(beyond[dr])
            def _():
                for k in reversed(range(pairs)):
                    for m in moves[d, k]:
                        m.start()

    def received_rows(group):
        for d, dr in ((0, -1), (1, 1)):

            @pl.when(beyond[-dr])
            def _():
                settle(r.recv.at[group + d], strips)

    g_rows = row_moves(
        lambda d, k: r.gmain.at[k, 0 if d == 0 else half - 1],
        lambda d, k: r.gcorn.at[k, d],
        lambda d, k: r.grow.at[d, k],
        lambda d, k: r.gcorn_in.at[d, k],
        GROWS,
        core,
    )
    start_rows(g_rows)
    g_far = []
    for k in range(1, pairs):
        g_far.append(move(r.gcols.at[k], r.rcols.at[k - 1], GFAR, seat(k, core)))
        g_far.append(move(r.gmain.at[k], r.rmain.at[k - 1], GFAR, seat(k, core)))

    @pl.when(core == 0)
    def _():
        for m in g_far:
            m.start()

    for q in range(4):
        parts = [r.sp[c, q] for c in range(chunks)]
        mean = jnp.sum(functools.reduce(jnp.add, parts), axis=1, keepdims=True) / channels
        parts = [part - mean for part in parts]
        square = functools.reduce(jnp.add, [part * part for part in parts])
        inv = lax.rsqrt(jnp.sum(square, axis=1, keepdims=True) / channels + 1e-06)
        r.rstd[q] = jnp.broadcast_to(inv, (cells, LANES))
        for c in range(chunks):
            lane = slice(c * LANES, (c + 1) * LANES)
            hat = parts[c] * inv
            r.sp[c, q] = hat
            r.nb[q * cells : (q + 1) * cells, lane] = (
                hat * vector(r.gain, lane) + vector(r.lnb, lane)
            ).astype(jnp.bfloat16)

    fetched("win")
    for n in range(hid // BLOCK):
        lane = slice(n * BLOCK, (n + 1) * BLOCK)
        pre_all = jnp.dot(r.nb[...], r.win[:, lane], preferred_element_type=jnp.float32)
        bias = vector(r.bin_, lane)
        pooled = None
        for q in range(4):
            pre = pre_all[q * cells : (q + 1) * cells] + bias
            cdf = 0.5 + 0.5 * lax.erf(pre * math.sqrt(0.5))
            pdf = jnp.exp(pre * pre * -0.5) * (1.0 / math.sqrt(2.0 * math.pi))
            r.dg[q * cells : (q + 1) * cells, lane] = cdf + pre * pdf
            value = pre * cdf
            pooled = value if pooled is None else pooled + value
        r.hb[:, lane] = (pooled * 0.25).astype(jnp.bfloat16)
    @pl.when(core == 1)
    def _():
        for m in g_far:
            m.start()

    fetched("wout")
    branch = jnp.dot(r.hb[...], r.wout[...], preferred_element_type=jnp.float32)
    for c in range(chunks):
        lane = slice(c * LANES, (c + 1) * LANES)
        total = None
        for row in range(2):
            for parity in range(2):
                part = r.xpad[c, reach : reach + side, pl.ds(PAD + parity, half, stride=2), :]
                part = part.reshape(half, 2, half, LANES)[:, row]
                total = part if total is None else total + part
        mixed = vector(r.scale, lane) * (branch[:, lane] + vector(r.bout, lane))
        r.grid_p[2 : half + 2, inner, lane] = total * 0.25 + mixed.reshape(half, half, LANES)

    fetched("cw")
    rim = half + 2
    comp = None
    for a in range(3):
        for b in range(3):
            part = r.grid_p[a : a + rim, PAD - 2 + b : PAD - 2 + b + WIDE, :]
            part = part.reshape(rim * WIDE, channels).astype(jnp.bfloat16)
            part = jnp.dot(part, r.cw[a * 3 + b], preferred_element_type=jnp.float32)
            comp = part if comp is None else comp + part
    comp = comp.reshape(rim, WIDE, channels)
    r.amain[me] = comp[1 : half + 1, 1 : half + 1]
    for d, at in ((0, 0), (1, half + 1)):
        r.acols[me, d] = comp[1 : half + 1, at]
        r.erow[d] = comp[at, 1 : half + 1]
        r.ecorn[d, 0:1, :] = comp[at, 0:1]
        r.ecorn[d, 1:2, :] = comp[at, half + 1 : half + 2]

    t_rows = row_moves(
        lambda d, k: r.erow.at[d],
        lambda d, k: r.ecorn.at[d],
        lambda d, k: r.arow.at[d, me],
        lambda d, k: r.acorn.at[d, me],
        TROWS,
        1 - core,
    )
    start_rows(t_rows)
    t_far = []
    for k in range(1, pairs):
        t_far.append(move(r.acols.at[me], r.acols.at[me], TFAR, seat(k, 1 - core)))
        t_far.append(move(r.amain.at[me], r.amain.at[me], TFAR, seat(k, 1 - core)))
    t_near = [
        move(r.acols.at[me], r.acols.at[me], TNEAR, partner),
        move(r.amain.at[me], r.amain.at[me], TNEAR, partner),
    ]
    for m in t_far + t_near:
        m.start()

    fetched("image")
    image = r.image_ref[g]
    keep = {}
    for d, near in ((1, jnp.maximum(g - 1, 0)), (0, jnp.minimum(g + 1, groups - 1))):
        there = (g > 0) if d == 1 else (g < groups - 1)
        keep[d] = (r.image_ref[near] == image).astype(jnp.float32) * there.astype(jnp.float32)

    received_rows(GROWS)
    settle(r.recv.at[GFAR], main)
    def far(own, other):
        return total_of([own] + [other(k) for k in range(pairs - 1)])
    r.grid_g[1 : half + 1, inner, :] = far(r.gmain[0], lambda k: r.rmain[k])
    r.grid_g[1 : half + 1, PAD - 1, :] = far(r.gcols[0, 0], lambda k: r.rcols[k, 0])
    r.grid_g[1 : half + 1, PAD + half, :] = far(r.gcols[0, 1], lambda k: r.rcols[k, 1])
    for d, row in ((1, 0), (0, half + 1)):
        r.grid_g[row, inner, :] = total_of([r.grow[d, k] for k in range(pairs)]) * keep[d]
        corner = total_of([r.gcorn_in[d, k] for k in range(pairs)]) * keep[d]
        r.grid_g[row, PAD - 1 : PAD, :] = corner[0:1]
        r.grid_g[row, PAD + half : PAD + half + 1, :] = corner[1:2]

    grads = None
    for a in range(3):
        for b in range(3):
            part = r.grid_g[a : a + half, PAD - 1 + b : PAD - 1 + b + half, :]
            part = part.reshape(cells, channels).astype(jnp.bfloat16)
            part = nt_dot(part, r.cw[(2 - a) * 3 + 2 - b])
            grads = part if grads is None else grads + part
    grads = grads * 0.25
    for c in range(chunks):
        lane = slice(c * LANES, (c + 1) * LANES)
        r.gq[c] = grads[:, lane].reshape(half, half, LANES)
    scaled = (grads * vector(r.scale)).astype(jnp.bfloat16)

    for n in range(hid // BLOCK):
        lane = slice(n * BLOCK, (n + 1) * BLOCK)
        dh = nt_dot(scaled, r.wout[lane, :])
        for q in range(4):
            rows = slice(q * cells, (q + 1) * cells)
            r.dpb[rows, lane] = (dh * r.dg[rows, lane]).astype(jnp.bfloat16)
    dn_all = nt_dot(r.dpb[...], r.win[...])
    for q in range(4):
        dn = dn_all[q * cells : (q + 1) * cells] * vector(r.gain)
        parts = [dn[:, c * LANES : (c + 1) * LANES] for c in range(chunks)]
        first = jnp.sum(functools.reduce(jnp.add, parts), axis=1, keepdims=True) / channels
        cross = functools.reduce(jnp.add, [parts[c] * r.sp[c, q] for c in range(chunks)])
        second = jnp.sum(cross, axis=1, keepdims=True) / channels
        for c in range(chunks):
            back = r.rstd[q] * (parts[c] - first - r.sp[c, q] * second)
            back = back.reshape(half, half, LANES)
            for i in range(half):
                r.gpad[c, reach + 2 * i + q // 2, pl.ds(PAD + q % 2, half, stride=2), :] = back[i]

    def backward_conv(c):
        outs = depthwise(r.gpad, r.dww, c, taps, side, True)
        direct = jnp.broadcast_to(r.gq[c][:, None], (half, 2, half, LANES)).reshape(side, half, LANES)
        for parity in range(2):
            value = outs[parity] + direct
            for i in range(side):
                r.obuf[c, i, pl.ds(parity, half, stride=2), :] = value[i]

    for c in range(chunks - 1):
        backward_conv(c)

    received_rows(TROWS)
    settle(r.recv.at[TFAR], main)
    passed = []
    for k in range(1, pairs):
        who = seat(k, 1 - core)
        passed.append(move(r.acols.at[who], r.acols.at[who], PASS, partner))
        passed.append(move(r.amain.at[who], r.amain.at[who], PASS, partner))
    for m in passed:
        m.start()
    passed_rows = {}
    for d, dr in ((0, -1), (1, 1)):
        for k in range(pairs):
            who = seat(k, 1 - core)
            passed_rows[d, k] = (
                move(r.arow.at[d, who], r.arow.at[d, who], PROWS + d, partner),
                move(r.acorn.at[d, who], r.acorn.at[d, who], PROWS + d, partner),
            )

        @pl.when(beyond[-dr])
        def _():
            for k in range(pairs):
                for m in passed_rows[d, k]:
                    m.start()

    backward_conv(chunks - 1)

    settle(r.recv.at[TNEAR], tile + 2 * edge)
    settle(r.recv.at[PASS], main)
    received_rows(PROWS)

    settle(r.send.at[0], (peers - 1) * 8 * LANES + slots * tile + 3 * main + tile + 2 * edge)
    for d, dr in ((0, -1), (1, 1)):

        @pl.when(beyond[dr])
        def _():
            settle(r.send.at[1 + d], 2 * strips)

        @pl.when(beyond[-dr])
        def _():
            settle(r.send.at[3 + d], strips)

    chosen = [[wide(mask) for mask in masks_of(p, me)] for p in range(peers)]
    bias = vector(r.cb)
    for s in range(slots):
        total = None
        west = jnp.zeros((half, channels), jnp.float32)
        east = jnp.zeros((half, channels), jnp.float32)
        line = {d: jnp.zeros((half, channels), jnp.float32) for d in range(2)}
        tips = {d: [jnp.zeros((1, channels), jnp.float32) for _ in range(2)] for d in range(2)}
        for p in range(peers):
            mask = chosen[p][s]
            part = (r.amain[p] + bias) * mask
            total = part if total is None else total + part
            if p > 0:
                west = west + r.acols[p - 1, 1] * mask
            if p < peers - 1:
                east = east + r.acols[p + 1, 0] * mask
            for d in range(2):
                line[d] = line[d] + r.arow[d, p] * mask
                if p > 0:
                    tips[d][0] = tips[d][0] + r.acorn[d, p - 1, 1:2, :] * mask[:1]
                if p < peers - 1:
                    tips[d][1] = tips[d][1] + r.acorn[d, p + 1, 0:1, :] * mask[:1]
        r.tokout[s] = total
        r.tokout[s, :, 0, :] += west
        r.tokout[s, :, half - 1, :] += east
        for d, row in ((1, 0), (0, half - 1)):
            r.tokout[s, row] += line[d] * keep[d]
            r.tokout[s, row, 0:1, :] += tips[d][0] * keep[d]
            r.tokout[s, row, half - 1 : half, :] += tips[d][1] * keep[d]


def tail(obuf, tokout, tok_hbm, dx_hbm, sems):
    chunks = obuf.shape[0]
    copies = [pltpu.make_async_copy(tokout, tok_hbm, sems.at[chunks])]
    for c in range(chunks):
        copies.append(
            pltpu.make_async_copy(obuf.at[c], dx_hbm.at[:, :, c * LANES : (c + 1) * LANES], sems.at[c])
        )
    for copy in copies:
        copy.start()
    for copy in copies:
        copy.wait()


def solution(mesh):
    groups, peers = mesh.shape["group"], mesh.shape["peer"]

    def on_device(
        features, image_of_row, llm_peer, token_grads, dw_weight, dw_bias, ln_gain, ln_bias,
        w_in, b_in, w_out, b_out, layer_scale, comp_weight, comp_bias,
    ):
        side, width, channels = features.shape
        slots = token_grads.shape[0]
        hid = w_in.shape[1]
        taps = math.isqrt(dw_weight.shape[0])
        half = side // 2
        cells = half * half
        chunks = channels // LANES
        assert width == side and llm_peer.shape == (1, 1)
        f32, bf16 = jnp.float32, jnp.bfloat16
        padded = (chunks, side + 2 * (taps // 2), side + 2 * PAD, LANES)
        block = (half, half, channels)
        strip = (half, channels)
        tip = (2, channels)
        hbm = pl.BlockSpec(memory_space=pltpu.HBM)
        pairs = peers // 2
        assert peers == 2 * pairs and pairs > 1
        vmem = pl.BlockSpec(memory_space=pltpu.VMEM)

        def dma(count):
            return pltpu.SemaphoreType.DMA((count,))

        def buf(*shape, kind=f32):
            return pltpu.VMEM(shape, kind)

        inputs = (
            "image_hbm", "owner_hbm", "x_hbm", "tg_hbm", "dww_hbm", "dwb_hbm", "gain_hbm", "lnb_hbm",
            "win_hbm", "bin_hbm", "wout_hbm", "bout_hbm", "scale_hbm", "cw_hbm", "cb_hbm",
        )
        held = {
            "obuf": buf(chunks, side, side, LANES),
            "tokout": buf(slots, *block),
        }
        sent = (slots + 1) * cells * channels + 2 * half * channels + peers * 8 * LANES
        sent += 3 * (pairs - 1) * (cells + 2 * half) * channels
        span = max(sent, (side * side + taps * taps) * channels) // LANES
        scratch = {
            "xpad": buf(*padded),
            "gpad": buf(*padded),
            "dww": buf(chunks, taps * taps, LANES),
            "gq": buf(chunks, half, half, LANES),
            "dwb": buf(channels),
            "gain": buf(channels),
            "lnb": buf(channels),
            "bout": buf(channels),
            "scale": buf(channels),
            "cb": buf(channels),
            "bin_": buf(hid),
            "win": buf(*w_in.shape, kind=bf16),
            "wout": buf(*w_out.shape, kind=bf16),
            "cw": buf(*comp_weight.shape, kind=bf16),
            "tg": buf(slots, *block),
            "ntg": buf(slots, *block),
            "sp": buf(chunks, 4, cells, LANES),
            "rstd": buf(4, cells, LANES),
            "nb": buf(4 * cells, channels, kind=bf16),
            "dg": buf(4 * cells, hid),
            "hb": buf(cells, hid, kind=bf16),
            "dpb": buf(4 * cells, hid, kind=bf16),
            "table": buf(peers, 8, LANES, kind=jnp.int32),
            "gmain": buf(pairs, *block),
            "gcols": buf(pairs, 2, *strip),
            "gcorn": buf(pairs, 2, *tip),
            "rmain": buf(pairs - 1, *block),
            "rcols": buf(pairs - 1, 2, *strip),
            "grow": buf(2, pairs, *strip),
            "gcorn_in": buf(2, pairs, *tip),
            "grid_g": buf(half + 2, half + 2 * PAD, channels),
            "grid_p": buf(half + 4, half + 2 * PAD, channels),
            "erow": buf(2, *strip),
            "ecorn": buf(2, *tip),
            "amain": buf(peers, *block),
            "acols": buf(peers, 2, *strip),
            "arow": buf(2, peers, *strip),
            "acorn": buf(2, peers, *tip),
            "image_ref": pltpu.SMEM(image_of_row.shape, jnp.int32),
            "owner_ref": pltpu.SMEM((1, 1), jnp.int32),
            "in_sems": dma(8),
            "send": dma(5),
            "span": buf(span, 1, LANES),
            "recv": dma(12),
        }
        names = inputs + tuple(held) + tuple(scratch)
        state = pl.pallas_call(
            functools.partial(kernel, groups, peers, taps, names),
            out_shape=tuple(held.values()),
            in_specs=[hbm] * len(inputs),
            out_specs=(vmem,) * len(held),
            scratch_shapes=list(scratch.values()),
            compiler_params=pltpu.CompilerParams(collective_id=0, has_side_effects=True),
        )(
            image_of_row,
            llm_peer,
            features,
            token_grads.reshape((slots,) + block),
            dw_weight,
            dw_bias,
            ln_gain,
            ln_bias,
            w_in,
            b_in,
            w_out,
            b_out,
            layer_scale,
            comp_weight,
            comp_bias,
        )
        tokens, grads = pl.pallas_call(
            tail,
            out_shape=(
                jax.ShapeDtypeStruct((slots,) + block, f32),
                jax.ShapeDtypeStruct(features.shape, f32),
            ),
            in_specs=[vmem] * len(held),
            out_specs=(hbm, hbm),
            scratch_shapes=[dma(chunks + 1)],
            compiler_params=pltpu.CompilerParams(vmem_limit_bytes=16 << 20),
        )(*state)
        return tokens.reshape(slots, cells, channels), grads

    placed = [P()] * 15
    placed[0] = P("group", "peer", None)
    placed[2] = P(("group", "peer"), None)
    placed[3] = P(("group", "peer"), None, None)
    return jax.shard_map(
        on_device,
        mesh=mesh,
        in_specs=tuple(placed),
        out_specs=(P(("group", "peer"), None, None), P("group", "peer", None)),
        check_vma=False,
    )
```

```python
import functools
import math
import types

import jax
import jax.numpy as jnp
from jax import lax
from jax.experimental import pallas as pl
from jax.experimental.pallas import tpu as pltpu
from jax.sharding import PartitionSpec as P

MESH = pl.DeviceIdType.MESH
LANES = 128
PAD = 8
BLOCK = 256
WIDE = 16
TABLE, NEAR, GROWS, GFAR, TROWS, TFAR, TNEAR, PASS, PROWS, RAW, RELAY = 0, 1, 2, 4, 5, 7, 8, 9, 10, 12, 13
SENT_BY = (0, 0, 1, 2, 0, 1, 2, 0, 0, 0, 3, 4, 0, 0)


def nt_dot(a, b):
    return lax.dot_general(a, b, (((1,), (1,)), ((), ())), preferred_element_type=jnp.float32)


def depthwise(src, weight, chunk, taps, side, flip):
    half = side // 2
    reach = taps // 2
    outs = []
    for parity in range(2):
        total = None
        for b in range(taps):
            rows = src[chunk, :, pl.ds(PAD - reach + parity + b, half, stride=2), :]
            for a in range(taps):
                k = (taps - 1 - a) * taps + taps - 1 - b if flip else a * taps + b
                term = rows[a : a + side] * weight[chunk, k : k + 1, :]
                total = term if total is None else total + term
        outs.append(total)
    return outs


def kernel(groups, peers, taps, names, *refs):
    r = types.SimpleNamespace(**dict(zip(names, refs)))
    g = lax.axis_index("group")
    me = lax.axis_index("peer")
    side = r.x_hbm.shape[0]
    channels = r.x_hbm.shape[2]
    half = side // 2
    cells = half * half
    chunks = channels // LANES
    reach = taps // 2
    hid = r.win.shape[1]
    slots = r.tg.shape[0]
    pairs = peers // 2
    core = lax.rem(me, 2)
    partner = me + 1 - 2 * core
    inner = slice(PAD, PAD + half)

    def vector(ref, lane=slice(None)):
        return ref[lane].reshape(1, -1)

    def seat(k, which):
        return lax.rem(lax.div(me, 2) + k, pairs) * 2 + which

    beyond = {-1: g > 0, 1: g < groups - 1}

    for buf in (r.grow, r.gcorn_in, r.arow, r.acorn):
        buf[...] = jnp.zeros_like(buf)
    barrier = pltpu.get_barrier_semaphore()

    def greet(row, who):
        pl.semaphore_signal(barrier, inc=1, device_id={"group": row, "peer": who}, device_id_type=MESH)

    for k in range(1, peers):
        greet(g, lax.rem(me + k, peers))
    @pl.when(beyond[1])
    def _():
        greet(g + 1, me)

    copies = {}

    def fetch(name, *moves):
        sem = r.in_sems.at[len(copies)]
        copies[name] = [pltpu.make_async_copy(src, dst, sem) for src, dst in moves]
        for copy in copies[name]:
            copy.start()

    def settle(sem, elements):
        span = r.span.at[pl.ds(0, elements // LANES)]
        pltpu.make_async_copy(span, span, sem).wait()

    def fetched(name):
        if len(copies[name]) == 1:
            copies[name][0].wait()
        else:
            elements = sum(math.prod(copy.dst_ref.shape) for copy in copies[name])
            settle(r.in_sems.at[list(copies).index(name)], elements)

    fetch("owner", (r.owner_hbm, r.owner_ref))
    fetch("tg", (r.tg_hbm, r.tg))
    fetch(
        "small",
        (r.dwb_hbm, r.dwb),
        (r.gain_hbm, r.gain),
        (r.lnb_hbm, r.lnb),
        (r.bout_hbm, r.bout),
        (r.scale_hbm, r.scale),
        (r.cb_hbm, r.cb),
        (r.bin_hbm, r.bin_),
    )
    by_lane = []
    for c in range(chunks):
        lane = slice(c * LANES, (c + 1) * LANES)
        by_lane.append((r.dww_hbm.at[:, lane], r.dww.at[c]))
        by_lane.append((r.x_hbm.at[:, :, lane], r.xpad.at[c, reach : reach + side, PAD : PAD + side, :]))
    fetch("x", *by_lane)
    fetch("image", (r.image_hbm, r.image_ref))
    fetch("win", (r.win_hbm, r.win))
    fetch("wout", (r.wout_hbm, r.wout))
    fetch("cw", (r.cw_hbm, r.cw))

    def clear(buf):
        width = buf.shape[2]
        for c in range(chunks):
            buf[c, :reach] = jnp.zeros((reach, width, LANES), jnp.float32)
            buf[c, reach + side :] = jnp.zeros((reach, width, LANES), jnp.float32)
            buf[c, reach : reach + side, :PAD] = jnp.zeros((side, PAD, LANES), jnp.float32)
            buf[c, reach : reach + side, PAD + side :] = jnp.zeros((side, PAD, LANES), jnp.float32)

    clear(r.xpad)
    clear(r.gpad)
    r.grid_p[...] = jnp.zeros_like(r.grid_p)

    def move(src, dst, group, where, row=None):
        return pltpu.make_async_remote_copy(
            src_ref=src,
            dst_ref=dst,
            send_sem=r.send.at[SENT_BY[group]],
            recv_sem=r.recv.at[group],
            device_id={"group": g if row is None else row, "peer": where},
            device_id_type=MESH,
        )

    fetched("owner")
    r.table[me] = jnp.full((8, LANES), r.owner_ref[0, 0], jnp.int32)
    pl.semaphore_wait(barrier, peers - 1 + (g > 0).astype(jnp.int32))

    @pl.when(beyond[-1])
    def _():
        pl.semaphore_signal(r.hello, inc=1, device_id={"group": g - 1, "peer": me}, device_id_type=MESH)


    table_moves = [
        move(r.table.at[me], r.table.at[me], TABLE, lax.rem(me + k, peers)) for k in range(1, peers)
    ]
    for m in table_moves:
        m.start()
    fetched("tg")
    near_move = move(r.tg, r.ntg, NEAR, partner)
    near_move.start()
    upper = half // 2
    raw_moves = [move(r.tg.at[:, upper:], r.xtg.at[0, k - 1], RAW, seat(k, core)) for k in range(1, pairs)]
    for m in raw_moves:
        m.start()

    def forward_conv(c):
        outs = depthwise(r.xpad, r.dww, c, taps, side, False)
        bias = vector(r.dwb, slice(c * LANES, (c + 1) * LANES))
        for parity in range(2):
            part = (outs[parity] + bias).reshape(half, 2, half, LANES)
            for row in range(2):
                r.sp[c, row * 2 + parity] = part[:, row].reshape(cells, LANES)

    fetched("small")
    fetched("x")
    for c in range(chunks):
        forward_conv(c)
    tile = cells * channels
    edge = half * channels
    main = (pairs - 1) * (tile + 2 * edge)
    masked = (pairs - 1) * upper * 2 * (edge // 2 + channels)
    raw = (pairs - 1) * slots * (half - upper) * edge
    strips = pairs * (edge + 2 * channels)
    for q in range(4):
        parts = [r.sp[c, q] for c in range(chunks)]
        mean = jnp.sum(functools.reduce(jnp.add, parts), axis=1, keepdims=True) / channels
        parts = [part - mean for part in parts]
        square = functools.reduce(jnp.add, [part * part for part in parts])
        inv = lax.rsqrt(jnp.sum(square, axis=1, keepdims=True) / channels + 1e-06)
        r.rstd[q] = jnp.broadcast_to(inv, (cells, LANES))
        for c in range(chunks):
            lane = slice(c * LANES, (c + 1) * LANES)
            hat = parts[c] * inv
            r.sp[c, q] = hat
            r.nb[q * cells : (q + 1) * cells, lane] = (
                hat * vector(r.gain, lane) + vector(r.lnb, lane)
            ).astype(jnp.bfloat16)

    settle(r.recv.at[TABLE], (peers - 1) * 8 * LANES)
    settle(r.recv.at[NEAR], slots * tile)

    def masks_of(who, device):
        inside = jnp.logical_and(who >= 0, who < peers)
        at = jnp.clip(who, 0, peers - 1)
        mine = jnp.logical_and(r.table[at] == device, inside)
        before = jnp.zeros((8, LANES), jnp.int32)
        for p in range(peers):
            earlier = (p < at).astype(jnp.int32)
            before = before + jnp.where(r.table[p] == device, earlier, 0)
        return [jnp.logical_and(mine, before == s).astype(jnp.float32) for s in range(slots)]

    def wide(mask):
        return jnp.concatenate([mask] * chunks, axis=1)

    def held(who):
        pairs_of = []
        for ref, device in ((r.tg, me), (r.ntg, partner)):
            for s, mask in enumerate(masks_of(who, device)):
                pairs_of.append((ref.at[s], wide(mask)))
        return pairs_of

    def held_far(who):
        pairs_of = []
        for k in range(1, pairs):
            for via, which in ((0, core), (1, 1 - core)):
                for s, mask in enumerate(masks_of(who, seat(pairs - k, which))):
                    pairs_of.append((r.xtg.at[via, k - 1, s], wide(mask)))
        return pairs_of

    def total_of(terms):
        return functools.reduce(jnp.add, terms)

    for k in range(pairs):
        home = seat(k, core)
        whole = held(home)
        for part in ((slice(0, half),) if k == 0 else (slice(0, upper), slice(half - 1, half))):
            r.gmain[k, part] = total_of([ref[part] * mask for ref, mask in whole])
        left = total_of([ref[:, half - 1, :] * mask for ref, mask in held(home - 1)])
        right = total_of([ref[:, 0, :] * mask for ref, mask in held(home + 1)])
        for side_at, col in ((0, left), (1, right)):
            if k == 0:
                r.gcols[side_at] = col
            else:
                r.gfar[k - 1, side_at] = col[:upper]
            for d, at in ((0, 0), (1, half - 1)):
                r.gcorn[k, d, side_at : side_at + 1, :] = col[at : at + 1]

    def row_moves(src_row, src_corner, dst_row, dst_corner, group, which):
        moves = {}
        for d, dr in ((0, -1), (1, 1)):
            for k in range(pairs):
                moves[d, k] = (
                    move(src_row(d, k), dst_row(d, k), group + d, seat(k, which), g + dr),
                    move(src_corner(d, k), dst_corner(d, k), group + d, seat(k, which), g + dr),
                )
        return moves

    def start_rows(moves):
        for d, dr in ((0, -1), (1, 1)):

            @pl.when(beyond[dr])
            def _():
                for k in reversed(range(pairs)):
                    for m in moves[d, k]:
                        m.start()

    def received_rows(group):
        for d, dr in ((0, -1), (1, 1)):

            @pl.when(beyond[-dr])
            def _():
                settle(r.recv.at[group + d], strips)

    g_rows = row_moves(
        lambda d, k: r.gmain.at[k, 0 if d == 0 else half - 1],
        lambda d, k: r.gcorn.at[k, d],
        lambda d, k: r.grow.at[d, k],
        lambda d, k: r.gcorn_in.at[d, k],
        GROWS,
        core,
    )
    @pl.when(beyond[1])
    def _():
        pl.semaphore_wait(r.hello, 1)

    start_rows(g_rows)
    g_far = []
    for k in range(1, pairs):
        g_far.append(move(r.gfar.at[k - 1], r.rcols.at[k - 1], GFAR, seat(k, core)))
        g_far.append(move(r.gmain.at[k, :upper], r.rmain.at[k - 1], GFAR, seat(k, core)))

    for m in g_far:
        m.start()

    fetched("win")
    for n in range(hid // BLOCK):
        lane = slice(n * BLOCK, (n + 1) * BLOCK)
        pre_all = jnp.dot(r.nb[...], r.win[:, lane], preferred_element_type=jnp.float32)
        bias = vector(r.bin_, lane)
        pooled = None
        for q in range(4):
            pre = pre_all[q * cells : (q + 1) * cells] + bias
            cdf = 0.5 + 0.5 * lax.erf(pre * math.sqrt(0.5))
            pdf = jnp.exp(pre * pre * -0.5) * (1.0 / math.sqrt(2.0 * math.pi))
            r.dg[q * cells : (q + 1) * cells, lane] = cdf + pre * pdf
            value = pre * cdf
            pooled = value if pooled is None else pooled + value
        r.hb[:, lane] = (pooled * 0.25).astype(jnp.bfloat16)
    fetched("wout")
    branch = jnp.dot(r.hb[...], r.wout[...], preferred_element_type=jnp.float32)
    for c in range(chunks):
        lane = slice(c * LANES, (c + 1) * LANES)
        total = None
        for row in range(2):
            for parity in range(2):
                part = r.xpad[c, reach : reach + side, pl.ds(PAD + parity, half, stride=2), :]
                part = part.reshape(half, 2, half, LANES)[:, row]
                total = part if total is None else total + part
        mixed = vector(r.scale, lane) * (branch[:, lane] + vector(r.bout, lane))
        r.grid_p[2 : half + 2, inner, lane] = total * 0.25 + mixed.reshape(half, half, LANES)

    r.grid_p[2 : half + 2, PAD + WIDE, :] = r.grid_p[2 : half + 2, PAD, :]
    fetched("cw")
    rim = half + 2
    for a in range(3):
        for b in range(3):
            part = r.grid_p[a : a + rim, PAD - 1 + b : PAD - 1 + b + WIDE, :]
            at = (a * 3 + b) * channels
            r.lhs[:, at : at + channels] = part.reshape(rim * WIDE, channels).astype(jnp.bfloat16)

    t_rows = row_moves(
        lambda d, k: r.erow.at[d],
        lambda d, k: r.ecorn.at[d],
        lambda d, k: r.arow.at[d, me],
        lambda d, k: r.acorn.at[d, me],
        TROWS,
        1 - core,
    )
    t_far = []
    spans = [slice(at, min(at + 3 * LANES, channels)) for at in range(0, channels, 3 * LANES)]
    for lane in spans:
        comp = jnp.dot(r.lhs[...], r.cw[:, lane], preferred_element_type=jnp.float32)
        comp = comp.reshape(rim, WIDE, -1)
        r.amain[me, :, :, lane] = comp[1 : half + 1, :half]
        r.beside[:, :, lane] = comp[:, half:]
        for d, at, col in ((0, 0, WIDE - 1 - half), (1, half + 1, 0)):
            r.acols[me, d, :, lane] = r.beside[1 : half + 1, col, lane]
            r.erow[d, :, lane] = comp[at, :half]
            r.ecorn[d, 0:1, lane] = r.beside[at, WIDE - 1 - half : WIDE - half, lane]
            r.ecorn[d, 1:2, lane] = r.beside[at, 0:1, lane]
        sends = []
        for k in range(1, pairs):
            for ref in (r.acols.at[me, :, :, lane], r.amain.at[me, :, :, lane]):
                sends.append(move(ref, ref, TFAR, seat(k, 1 - core)))
        if lane is spans[-1]:
            start_rows(t_rows)
        for m in sends:
            m.start()
        t_far += sends
    t_near = [
        move(r.acols.at[me], r.acols.at[me], TNEAR, partner),
        move(r.amain.at[me], r.amain.at[me], TNEAR, partner),
    ]
    for m in t_near:
        m.start()

    settle(r.recv.at[RAW], raw)
    relay = move(r.xtg.at[0], r.xtg.at[1], RELAY, partner)
    relay.start()

    for a in range(3):
        for b in range(3):
            at, flipped = (a * 3 + b) * channels, ((2 - a) * 3 + 2 - b) * channels
            r.cwt[at : at + channels] = r.cw[flipped : flipped + channels].T

    fetched("image")
    image = r.image_ref[g]
    keep = {}
    for d, near in ((1, jnp.maximum(g - 1, 0)), (0, jnp.minimum(g + 1, groups - 1))):
        there = (g > 0) if d == 1 else (g < groups - 1)
        keep[d] = (r.image_ref[near] == image).astype(jnp.float32) * there.astype(jnp.float32)

    settle(r.recv.at[RELAY], raw)
    lower = slice(upper, half)
    r.grid_g[1 + upper : half + 1, inner, :] = total_of(
        [r.gmain[0, lower]] + [ref[...] * mask for ref, mask in held_far(me)]
    )
    for side_at, who, col, at in ((0, me - 1, half - 1, PAD - 1), (1, me + 1, 0, PAD + half)):
        r.grid_g[1 + upper : half + 1, at, :] = total_of(
            [r.gcols[side_at, lower]] + [ref[:, col, :] * mask[: half - upper] for ref, mask in held_far(who)]
        )
    received_rows(GROWS)
    settle(r.recv.at[GFAR], masked)
    r.grid_g[1 : 1 + upper, inner, :] = total_of([r.gmain[0, :upper]] + [r.rmain[k] for k in range(pairs - 1)])
    for side_at, at in ((0, PAD - 1), (1, PAD + half)):
        r.grid_g[1 : 1 + upper, at, :] = total_of(
            [r.gcols[side_at, :upper]] + [r.rcols[k, side_at] for k in range(pairs - 1)]
        )
    for d, row in ((1, 0), (0, half + 1)):
        r.grid_g[row, inner, :] = total_of([r.grow[d, k] for k in range(pairs)]) * keep[d]
        corner = total_of([r.gcorn_in[d, k] for k in range(pairs)]) * keep[d]
        r.grid_g[row, PAD - 1 : PAD, :] = corner[0:1]
        r.grid_g[row, PAD + half : PAD + half + 1, :] = corner[1:2]

    for a in range(3):
        for b in range(3):
            part = r.grid_g[a : a + half, PAD - 1 + b : PAD - 1 + b + half, :]
            at = (a * 3 + b) * channels
            r.lhs[:cells, at : at + channels] = part.reshape(cells, channels).astype(jnp.bfloat16)
    grads = jnp.dot(r.lhs[:cells], r.cwt[...], preferred_element_type=jnp.float32)
    grads = grads * 0.25
    for c in range(chunks):
        lane = slice(c * LANES, (c + 1) * LANES)
        r.gq[c] = grads[:, lane].reshape(half, half, LANES)
    scaled = (grads * vector(r.scale)).astype(jnp.bfloat16)

    for n in range(hid // BLOCK):
        lane = slice(n * BLOCK, (n + 1) * BLOCK)
        dh = nt_dot(scaled, r.wout[lane, :])
        for q in range(4):
            rows = slice(q * cells, (q + 1) * cells)
            r.dpb[rows, lane] = (dh * r.dg[rows, lane]).astype(jnp.bfloat16)
    dn_all = nt_dot(r.dpb[...], r.win[...])
    for q in range(4):
        dn = dn_all[q * cells : (q + 1) * cells] * vector(r.gain)
        parts = [dn[:, c * LANES : (c + 1) * LANES] for c in range(chunks)]
        first = jnp.sum(functools.reduce(jnp.add, parts), axis=1, keepdims=True) / channels
        cross = functools.reduce(jnp.add, [parts[c] * r.sp[c, q] for c in range(chunks)])
        second = jnp.sum(cross, axis=1, keepdims=True) / channels
        for c in range(chunks):
            back = r.rstd[q] * (parts[c] - first - r.sp[c, q] * second)
            back = back.reshape(half, half, LANES)
            for i in range(half):
                r.gpad[c, reach + 2 * i + q // 2, pl.ds(PAD + q % 2, half, stride=2), :] = back[i]

    def backward_conv(c):
        outs = depthwise(r.gpad, r.dww, c, taps, side, True)
        direct = jnp.broadcast_to(r.gq[c][:, None], (half, 2, half, LANES)).reshape(side, half, LANES)
        for parity in range(2):
            value = outs[parity] + direct
            for i in range(side):
                r.obuf[c, i, pl.ds(parity, half, stride=2), :] = value[i]

    backward_conv(0)

    received_rows(TROWS)
    settle(r.recv.at[TFAR], main)
    passed = []
    for k in range(1, pairs):
        who = seat(k, 1 - core)
        passed.append(move(r.acols.at[who], r.acols.at[who], PASS, partner))
        passed.append(move(r.amain.at[who], r.amain.at[who], PASS, partner))
    for m in passed:
        m.start()
    passed_rows = {}
    for d, dr in ((0, -1), (1, 1)):
        for k in range(pairs):
            who = seat(k, 1 - core)
            passed_rows[d, k] = (
                move(r.arow.at[d, who], r.arow.at[d, who], PROWS + d, partner),
                move(r.acorn.at[d, who], r.acorn.at[d, who], PROWS + d, partner),
            )

        @pl.when(beyond[-dr])
        def _():
            for k in range(pairs):
                for m in passed_rows[d, k]:
                    m.start()

    for c in range(1, chunks):
        backward_conv(c)

    settle(r.recv.at[TNEAR], tile + 2 * edge)
    settle(r.recv.at[PASS], main)
    received_rows(PROWS)

    settle(r.send.at[0], (peers - 1) * 8 * LANES + slots * tile + 2 * raw + masked + 2 * main + tile + 2 * edge)
    for d, dr in ((0, -1), (1, 1)):

        @pl.when(beyond[dr])
        def _():
            settle(r.send.at[1 + d], 2 * strips)

        @pl.when(beyond[-dr])
        def _():
            settle(r.send.at[3 + d], strips)

    chosen = [[wide(mask) for mask in masks_of(p, me)] for p in range(peers)]
    bias = vector(r.cb)
    for s in range(slots):
        total = None
        west = jnp.zeros((half, channels), jnp.float32)
        east = jnp.zeros((half, channels), jnp.float32)
        line = {d: jnp.zeros((half, channels), jnp.float32) for d in range(2)}
        tips = {d: [jnp.zeros((1, channels), jnp.float32) for _ in range(2)] for d in range(2)}
        for p in range(peers):
            mask = chosen[p][s]
            part = (r.amain[p] + bias) * mask
            total = part if total is None else total + part
            if p > 0:
                west = west + r.acols[p - 1, 1] * mask
            if p < peers - 1:
                east = east + r.acols[p + 1, 0] * mask
            for d in range(2):
                line[d] = line[d] + r.arow[d, p] * mask
                if p > 0:
                    tips[d][0] = tips[d][0] + r.acorn[d, p - 1, 1:2, :] * mask[:1]
                if p < peers - 1:
                    tips[d][1] = tips[d][1] + r.acorn[d, p + 1, 0:1, :] * mask[:1]
        r.tokout[s] = total
        r.tokout[s, :, 0, :] += west
        r.tokout[s, :, half - 1, :] += east
        for d, row in ((1, 0), (0, half - 1)):
            r.tokout[s, row] += line[d] * keep[d]
            r.tokout[s, row, 0:1, :] += tips[d][0] * keep[d]
            r.tokout[s, row, half - 1 : half, :] += tips[d][1] * keep[d]


def tail(obuf, tokout, tok_hbm, dx_hbm, sems):
    chunks = obuf.shape[0]
    copies = [pltpu.make_async_copy(tokout, tok_hbm, sems.at[chunks])]
    for c in range(chunks):
        copies.append(
            pltpu.make_async_copy(obuf.at[c], dx_hbm.at[:, :, c * LANES : (c + 1) * LANES], sems.at[c])
        )
    for copy in copies:
        copy.start()
    for copy in copies:
        copy.wait()


def solution(mesh):
    groups, peers = mesh.shape["group"], mesh.shape["peer"]

    def on_device(
        features, image_of_row, llm_peer, token_grads, dw_weight, dw_bias, ln_gain, ln_bias,
        w_in, b_in, w_out, b_out, layer_scale, comp_weight, comp_bias,
    ):
        side, width, channels = features.shape
        slots = token_grads.shape[0]
        hid = w_in.shape[1]
        taps = math.isqrt(dw_weight.shape[0])
        half = side // 2
        cells = half * half
        chunks = channels // LANES
        assert width == side and llm_peer.shape == (1, 1)
        f32, bf16 = jnp.float32, jnp.bfloat16
        padded = (chunks, side + 2 * (taps // 2), side + 2 * PAD, LANES)
        block = (half, half, channels)
        strip = (half, channels)
        tip = (2, channels)
        hbm = pl.BlockSpec(memory_space=pltpu.HBM)
        pairs = peers // 2
        assert peers == 2 * pairs and pairs > 1
        vmem = pl.BlockSpec(memory_space=pltpu.VMEM)

        def dma(count):
            return pltpu.SemaphoreType.DMA((count,))

        def buf(*shape, kind=f32):
            return pltpu.VMEM(shape, kind)

        inputs = (
            "image_hbm", "owner_hbm", "x_hbm", "tg_hbm", "dww_hbm", "dwb_hbm", "gain_hbm", "lnb_hbm",
            "win_hbm", "bin_hbm", "wout_hbm", "bout_hbm", "scale_hbm", "cw_hbm", "cb_hbm",
        )
        held = {
            "obuf": buf(chunks, side, side, LANES),
            "tokout": buf(slots, *block),
        }
        sent = (slots + 1) * cells * channels + 2 * half * channels + peers * 8 * LANES
        sent += (pairs - 1) * (3 * (cells + 2 * half) + 2 * slots * cells) * channels
        span = max(sent, (side * side + taps * taps) * channels) // LANES
        scratch = {
            "xpad": buf(*padded),
            "gpad": buf(*padded),
            "dww": buf(chunks, taps * taps, LANES),
            "gq": buf(chunks, half, half, LANES),
            "dwb": buf(channels),
            "gain": buf(channels),
            "lnb": buf(channels),
            "bout": buf(channels),
            "scale": buf(channels),
            "cb": buf(channels),
            "bin_": buf(hid),
            "win": buf(*w_in.shape, kind=bf16),
            "wout": buf(*w_out.shape, kind=bf16),
            "cw": buf(9 * channels, channels, kind=bf16),
            "cwt": buf(9 * channels, channels, kind=bf16),
            "lhs": buf((half + 2) * WIDE, 9 * channels, kind=bf16),
            "tg": buf(slots, *block),
            "ntg": buf(slots, *block),
            "sp": buf(chunks, 4, cells, LANES),
            "rstd": buf(4, cells, LANES),
            "nb": buf(4 * cells, channels, kind=bf16),
            "dg": buf(4 * cells, hid),
            "hb": buf(cells, hid, kind=bf16),
            "dpb": buf(4 * cells, hid, kind=bf16),
            "table": buf(peers, 8, LANES, kind=jnp.int32),
            "gmain": buf(pairs, *block),
            "gcols": buf(2, *strip),
            "gfar": buf(pairs - 1, 2, half // 2, channels),
            "xtg": buf(2, pairs - 1, slots, half - half // 2, half, channels),
            "gcorn": buf(pairs, 2, *tip),
            "rmain": buf(pairs - 1, half // 2, half, channels),
            "rcols": buf(pairs - 1, 2, half // 2, channels),
            "grow": buf(2, pairs, *strip),
            "gcorn_in": buf(2, pairs, *tip),
            "grid_g": buf(half + 2, half + 2 * PAD, channels),
            "grid_p": buf(half + 4, PAD + WIDE + PAD, channels),
            "beside": buf(half + 2, WIDE - half, channels),
            "erow": buf(2, *strip),
            "ecorn": buf(2, *tip),
            "amain": buf(peers, *block),
            "acols": buf(peers, 2, *strip),
            "arow": buf(2, peers, *strip),
            "acorn": buf(2, peers, *tip),
            "image_ref": pltpu.SMEM(image_of_row.shape, jnp.int32),
            "owner_ref": pltpu.SMEM((1, 1), jnp.int32),
            "in_sems": dma(8),
            "hello": pltpu.SemaphoreType.REGULAR,
            "send": dma(5),
            "span": buf(span, 1, LANES),
            "recv": dma(14),
        }
        names = inputs + tuple(held) + tuple(scratch)
        state = pl.pallas_call(
            functools.partial(kernel, groups, peers, taps, names),
            out_shape=tuple(held.values()),
            in_specs=[hbm] * len(inputs),
            out_specs=(vmem,) * len(held),
            scratch_shapes=list(scratch.values()),
            compiler_params=pltpu.CompilerParams(collective_id=0, has_side_effects=True),
        )(
            image_of_row,
            llm_peer,
            features,
            token_grads.reshape((slots,) + block),
            dw_weight,
            dw_bias,
            ln_gain,
            ln_bias,
            w_in,
            b_in,
            w_out,
            b_out,
            layer_scale,
            comp_weight.reshape(9 * channels, channels),
            comp_bias,
        )
        tokens, grads = pl.pallas_call(
            tail,
            out_shape=(
                jax.ShapeDtypeStruct((slots,) + block, f32),
                jax.ShapeDtypeStruct(features.shape, f32),
            ),
            in_specs=[vmem] * len(held),
            out_specs=(hbm, hbm),
            scratch_shapes=[dma(chunks + 1)],
            compiler_params=pltpu.CompilerParams(vmem_limit_bytes=16 << 20),
        )(*state)
        return tokens.reshape(slots, cells, channels), grads

    placed = [P()] * 15
    placed[0] = P("group", "peer", None)
    placed[2] = P(("group", "peer"), None)
    placed[3] = P(("group", "peer"), None, None)
    return jax.shard_map(
        on_device,
        mesh=mesh,
        in_specs=tuple(placed),
        out_specs=(P(("group", "peer"), None, None), P("group", "peer", None)),
        check_vma=False,
    )
```

```python
import functools
import math
import types

import jax
import jax.numpy as jnp
from jax import lax
from jax.experimental import pallas as pl
from jax.experimental.pallas import tpu as pltpu
from jax.sharding import PartitionSpec as P

MESH = pl.DeviceIdType.MESH
LANES = 128
PAD = 8
BLOCK = 256
WIDE = 16
TABLE, GROWS, GFAR, TROWS, TFAR, PASS, PROWS, RAW, RELAY = 0, 1, 3, 4, 6, 8, 9, 11, 12
SENT_BY = (0, 1, 2, 0, 1, 2, 0, 0, 0, 3, 4, 0, 0)


def nt_dot(a, b):
    return lax.dot_general(a, b, (((1,), (1,)), ((), ())), preferred_element_type=jnp.float32)


def depthwise_taps(weight, table, chunk, taps, flip):
    h = [weight[chunk, a * taps : (a + 1) * taps, :] for a in range(taps)]
    if flip:
        h = h[::-1]
    s = [h[0] + h[1], h[2] + h[3], h[4] + h[5], h[6]]
    rows = [s[0], s[2], s[1], s[3], s[0] + s[1], s[2] + s[3]]
    rows += [h[0], h[4], h[2], h[6], h[0] + h[2], h[4] + h[6], h[1], h[3], h[5]]
    for t, row in enumerate(rows):
        table[chunk, t, :taps] = row


def depthwise(src, sums, table, chunk, taps, side, flip):
    half = side // 2
    reach = taps // 2
    pairs = (side + taps - 1) // 2
    quads = pairs // 2
    for i in range(pairs):
        sums[i] = src[chunk, 2 * i] + src[chunk, 2 * i + 1]
    for i in range(quads):
        sums[pairs + i] = sums[2 * i] + sums[2 * i + 1]
        sums[pairs + quads + i] = src[chunk, 4 * i + 1] + src[chunk, 4 * i + 3]

    outs = []
    for parity in range(2):

        def leaf(row, tap_ids, count):
            totals = [None] * count
            for b in range(taps):
                cols = pl.ds(PAD - reach + parity + b, half, stride=2)
                at = taps - 1 - b if flip else b
                lines = [row(i, cols) for i in range(count + len(tap_ids) - 1)]
                for j, t in enumerate(tap_ids):
                    tap = table[chunk, t, at : at + 1, :]
                    for i in range(count):
                        term = lines[i + j] * tap
                        totals[i] = term if totals[i] is None else totals[i] + term
            return totals

        def nested(odd, even, both, first):
            n = half // 2
            f = leaf(odd, (first, first + 1), n)
            g = leaf(even, (first + 2, first + 3), n + 1)
            s = leaf(both, (first + 4, first + 5), n)
            return [f[i // 2] + g[i // 2 + 1] if i % 2 else s[i // 2] - f[i // 2] - g[i // 2] for i in range(half)]

        s = nested(
            lambda i, cols: sums[2 * i + 1, cols, :],
            lambda i, cols: sums[2 * i, cols, :],
            lambda i, cols: sums[pairs + i, cols, :],
            0,
        )
        f = nested(
            lambda i, cols: src[chunk, 4 * i + 3, cols, :],
            lambda i, cols: src[chunk, 4 * i + 1, cols, :],
            lambda i, cols: sums[pairs + quads + i, cols, :],
            6,
        )
        g = leaf(lambda i, cols: src[chunk, 2 * i, cols, :], (12, 13, 14), half + 1)
        outs.append([f[i // 2] + g[i // 2 + 1] if i % 2 else s[i // 2] - f[i // 2] - g[i // 2] for i in range(side)])
    return outs


def kernel(groups, peers, taps, names, *refs):
    r = types.SimpleNamespace(**dict(zip(names, refs)))
    g = lax.axis_index("group")
    me = lax.axis_index("peer")
    side = r.x_hbm.shape[0]
    channels = r.x_hbm.shape[2]
    half = side // 2
    cells = half * half
    chunks = channels // LANES
    reach = taps // 2
    hid = r.win.shape[1]
    slots = r.tg.shape[0]
    pairs = peers // 2
    core = lax.rem(me, 2)
    partner = me + 1 - 2 * core
    inner = slice(PAD, PAD + half)

    def vector(ref, lane=slice(None)):
        return ref[lane].reshape(1, -1)

    def seat(k, which):
        return lax.rem(lax.div(me, 2) + k, pairs) * 2 + which

    def across(k):
        return seat(k, core if k == 0 else 1 - core)

    beyond = {-1: g > 0, 1: g < groups - 1}

    for buf in (r.grow, r.gcorn_in, r.arow, r.acorn):
        buf[...] = jnp.zeros_like(buf)
    barrier = pltpu.get_barrier_semaphore()

    def greet(row, who):
        pl.semaphore_signal(barrier, inc=1, device_id={"group": row, "peer": who}, device_id_type=MESH)

    for k in range(1, peers):
        greet(g, lax.rem(me + k, peers))
    @pl.when(beyond[1])
    def _():
        greet(g + 1, me)

    copies = {}

    def fetch(name, *moves):
        sem = r.in_sems.at[len(copies)]
        copies[name] = [pltpu.make_async_copy(src, dst, sem) for src, dst in moves]
        for copy in copies[name]:
            copy.start()

    def settle(sem, elements):
        span = r.span.at[pl.ds(0, elements // LANES)]
        pltpu.make_async_copy(span, span, sem).wait()

    def fetched(name):
        if len(copies[name]) == 1:
            copies[name][0].wait()
        else:
            elements = sum(math.prod(copy.dst_ref.shape) for copy in copies[name])
            settle(r.in_sems.at[list(copies).index(name)], elements)

    fetch("owner", (r.owner_hbm, r.owner_ref))
    fetch("tg", (r.tg_hbm, r.tg))
    by_lane = []
    for c in range(chunks):
        lane = slice(c * LANES, (c + 1) * LANES)
        by_lane.append((r.dww_hbm.at[:, lane], r.dww.at[c]))
        by_lane.append((r.x_hbm.at[:, :, lane], r.xpad.at[c, reach : reach + side, PAD : PAD + side, :]))
    fetch(
        "x",
        *by_lane,
        (r.dwb_hbm, r.dwb),
        (r.gain_hbm, r.gain),
        (r.lnb_hbm, r.lnb),
        (r.bout_hbm, r.bout),
        (r.scale_hbm, r.scale),
        (r.cb_hbm, r.cb),
        (r.bin_hbm, r.bin_),
    )
    fetch("image", (r.image_hbm, r.image_ref))
    fetch("win", (r.win_hbm, r.win))
    fetch("wout", (r.wout_hbm, r.wout))
    fetch("cw", (r.cw_hbm, r.cw))

    def clear(buf):
        width = buf.shape[2]
        for c in range(chunks):
            buf[c, :reach] = jnp.zeros((reach, width, LANES), jnp.float32)
            buf[c, reach + side :] = jnp.zeros((reach, width, LANES), jnp.float32)
            buf[c, reach : reach + side, :PAD] = jnp.zeros((side, PAD, LANES), jnp.float32)
            buf[c, reach : reach + side, PAD + side :] = jnp.zeros((side, PAD, LANES), jnp.float32)

    clear(r.xpad)
    clear(r.gpad)
    r.grid_p[...] = jnp.zeros_like(r.grid_p)

    def move(src, dst, group, where, row=None):
        return pltpu.make_async_remote_copy(
            src_ref=src,
            dst_ref=dst,
            send_sem=r.send.at[SENT_BY[group]],
            recv_sem=r.recv.at[group],
            device_id={"group": g if row is None else row, "peer": where},
            device_id_type=MESH,
        )

    fetched("owner")
    r.table[me] = jnp.full((8, LANES), r.owner_ref[0, 0], jnp.int32)
    pl.semaphore_wait(barrier, peers - 1 + (g > 0).astype(jnp.int32))

    @pl.when(beyond[-1])
    def _():
        pl.semaphore_signal(r.hello, inc=1, device_id={"group": g - 1, "peer": me}, device_id_type=MESH)


    table_moves = [
        move(r.table.at[me], r.table.at[me], TABLE, lax.rem(me + k, peers)) for k in range(1, peers)
    ]
    for m in table_moves:
        m.start()
    fetched("tg")
    near_move = move(r.tg, r.ntg, TABLE, partner)
    near_move.start()
    upper = half // 2
    raw_moves = [move(r.tg.at[:, upper:], r.xtg.at[0, k - 1], RAW, across(k)) for k in range(1, pairs)]
    for m in raw_moves:
        m.start()

    def forward_conv(c):
        depthwise_taps(r.dww, r.taps, c, taps, False)
        outs = depthwise(r.xpad, r.sums, r.taps, c, taps, side, False)
        bias = vector(r.dwb, slice(c * LANES, (c + 1) * LANES))
        for parity in range(2):
            for i in range(side):
                at = i // 2 * half
                r.sp[c, i % 2 * 2 + parity, at : at + half] = outs[parity][i] + bias

    fetched("x")
    for c in range(chunks):
        forward_conv(c)
    def gelu(n):
        lane = slice(n * BLOCK, (n + 1) * BLOCK)
        pre_all = jnp.dot(r.nb[...], r.win[:, lane], preferred_element_type=jnp.float32)
        bias = vector(r.bin_, lane)
        pooled = None
        for q in range(4):
            pre = pre_all[q * cells : (q + 1) * cells] + bias
            cdf = 0.5 + 0.5 * lax.erf(pre * math.sqrt(0.5))
            pdf = jnp.exp(pre * pre * -0.5) * (1.0 / math.sqrt(2.0 * math.pi))
            r.dg[q * cells : (q + 1) * cells, lane] = cdf + pre * pdf
            value = pre * cdf
            pooled = value if pooled is None else pooled + value
        r.hb[:, lane] = (pooled * 0.25).astype(jnp.bfloat16)

    tile = cells * channels
    edge = half * channels
    main = (pairs - 1) * (tile + 2 * edge)
    masked = (pairs - 1) * (upper * edge + half * channels)
    raw = (pairs - 1) * slots * (half - upper) * edge
    strips = pairs * (edge + 2 * channels)
    for q in range(4):
        parts = [r.sp[c, q] for c in range(chunks)]
        mean = jnp.sum(functools.reduce(jnp.add, parts), axis=1, keepdims=True) / channels
        parts = [part - mean for part in parts]
        square = functools.reduce(jnp.add, [part * part for part in parts])
        inv = lax.rsqrt(jnp.sum(square, axis=1, keepdims=True) / channels + 1e-06)
        r.rstd[q] = jnp.broadcast_to(inv, (cells, LANES))
        for c in range(chunks):
            lane = slice(c * LANES, (c + 1) * LANES)
            hat = parts[c] * inv
            r.sp[c, q] = hat
            r.nb[q * cells : (q + 1) * cells, lane] = (
                hat * vector(r.gain, lane) + vector(r.lnb, lane)
            ).astype(jnp.bfloat16)

    fetched("win")
    for n in range(hid // BLOCK):
        gelu(n)

    settle(r.recv.at[TABLE], (peers - 1) * 8 * LANES + slots * tile)

    def masks_of(who, device):
        inside = jnp.logical_and(who >= 0, who < peers)
        at = jnp.clip(who, 0, peers - 1)
        mine = jnp.logical_and(r.table[at] == device, inside)
        before = jnp.zeros((8, LANES), jnp.int32)
        for p in range(peers):
            earlier = (p < at).astype(jnp.int32)
            before = before + jnp.where(r.table[p] == device, earlier, 0)
        return [jnp.logical_and(mine, before == s).astype(jnp.float32) for s in range(slots)]

    def wide(mask):
        return jnp.concatenate([mask] * chunks, axis=1)

    def held(who):
        pairs_of = []
        for ref, device in ((r.tg, me), (r.ntg, partner)):
            for s, mask in enumerate(masks_of(who, device)):
                pairs_of.append((ref.at[s], wide(mask)))
        return pairs_of

    def held_far(who):
        pairs_of = []
        for k in range(1, pairs):
            for via, which in ((0, 1 - core), (1, core)):
                for s, mask in enumerate(masks_of(who, seat(pairs - k, which))):
                    pairs_of.append((r.xtg.at[via, k - 1, s], wide(mask)))
        return pairs_of

    def total_of(terms):
        return functools.reduce(jnp.add, terms)

    for k in range(pairs):
        home = across(k)
        whole = held(home)
        for part in ((slice(0, half),) if k == 0 else (slice(0, upper), slice(half - 1, half))):
            r.gmain[k, part] = total_of([ref[part] * mask for ref, mask in whole])
        left = total_of([ref[:, half - 1, :] * mask for ref, mask in held(home - 1)])
        right = total_of([ref[:, 0, :] * mask for ref, mask in held(home + 1)])
        for side_at, col in ((0, left), (1, right)):
            if k == 0:
                r.gcols[side_at] = col
            else:
                r.gfar[k - 1, side_at] = col[: half // 2]
            for d, at in ((0, 0), (1, half - 1)):
                r.gcorn[k, d, side_at : side_at + 1, :] = col[at : at + 1]

    def row_moves(src_row, src_corner, dst_row, dst_corner, group, where):
        moves = {}
        for d, dr in ((0, -1), (1, 1)):
            for k in range(pairs):
                moves[d, k] = (
                    move(src_row(d, k), dst_row(d, k), group + d, where(k), g + dr),
                    move(src_corner(d, k), dst_corner(d, k), group + d, where(k), g + dr),
                )
        return moves

    def start_rows(moves):
        for d, dr in ((0, -1), (1, 1)):

            @pl.when(beyond[dr])
            def _():
                for k in reversed(range(pairs)):
                    for m in moves[d, k]:
                        m.start()

    def received_rows(group):
        for d, dr in ((0, -1), (1, 1)):

            @pl.when(beyond[-dr])
            def _():
                settle(r.recv.at[group + d], strips)

    g_rows = row_moves(
        lambda d, k: r.gmain.at[k, 0 if d == 0 else half - 1],
        lambda d, k: r.gcorn.at[k, d],
        lambda d, k: r.grow.at[d, k],
        lambda d, k: r.gcorn_in.at[d, k],
        GROWS,
        across,
    )
    @pl.when(beyond[1])
    def _():
        pl.semaphore_wait(r.hello, 1)

    start_rows(g_rows)
    g_far = []
    for k in range(1, pairs):
        g_far.append(move(r.gfar.at[k - 1], r.rcols.at[k - 1], GFAR, across(k)))
        g_far.append(move(r.gmain.at[k, :upper], r.rmain.at[k - 1], GFAR, across(k)))

    for m in g_far:
        m.start()

    fetched("wout")
    branch = jnp.dot(r.hb[...], r.wout[...], preferred_element_type=jnp.float32)
    for c in range(chunks):
        lane = slice(c * LANES, (c + 1) * LANES)
        total = None
        for row in range(2):
            for parity in range(2):
                part = r.xpad[c, reach : reach + side, pl.ds(PAD + parity, half, stride=2), :]
                part = part.reshape(half, 2, half, LANES)[:, row]
                total = part if total is None else total + part
        mixed = vector(r.scale, lane) * (branch[:, lane] + vector(r.bout, lane))
        r.grid_p[2 : half + 2, inner, lane] = total * 0.25 + mixed.reshape(half, half, LANES)

    r.grid_p[2 : half + 2, PAD + WIDE, :] = r.grid_p[2 : half + 2, PAD, :]
    fetched("cw")
    rim = half + 2
    for a in range(3):
        for b in range(3):
            part = r.grid_p[a : a + rim, PAD - 1 + b : PAD - 1 + b + WIDE, :]
            at = (a * 3 + b) * channels
            r.lhs[:, at : at + channels] = part.reshape(rim * WIDE, channels).astype(jnp.bfloat16)

    t_rows = row_moves(
        lambda d, k: r.erow.at[d],
        lambda d, k: r.ecorn.at[d],
        lambda d, k: r.arow.at[d, me],
        lambda d, k: r.acorn.at[d, me],
        TROWS,
        lambda k: seat(k, 1 - core),
    )
    t_far = []
    spans = [slice(at, min(at + 3 * LANES, channels)) for at in range(0, channels, 3 * LANES)]
    for lane in spans:
        comp = jnp.dot(r.lhs[...], r.cw[:, lane], preferred_element_type=jnp.float32)
        comp = comp.reshape(rim, WIDE, -1)
        r.amain[me, :, :, lane] = comp[1 : half + 1, :half]
        r.beside[:, :, lane] = comp[:, half:]
        for d, at, col in ((0, 0, WIDE - 1 - half), (1, half + 1, 0)):
            r.acols[me, d, :, lane] = r.beside[1 : half + 1, col, lane]
            r.erow[d, :, lane] = comp[at, :half]
            r.ecorn[d, 0:1, lane] = r.beside[at, WIDE - 1 - half : WIDE - half, lane]
            r.ecorn[d, 1:2, lane] = r.beside[at, 0:1, lane]
        sends = []
        for k in range(1, pairs):
            for ref, group in (
                (r.acols.at[me, :, :, lane], TFAR),
                (r.amain.at[me, : half // 2, :, lane], TFAR),
                (r.amain.at[me, half // 2 :, :, lane], TFAR + 1),
            ):
                sends.append(move(ref, ref, group, seat(k, 1 - core)))
        if lane is spans[-1]:
            start_rows(t_rows)
        for m in sends:
            m.start()
        t_far += sends
    t_near = [
        move(r.acols.at[me], r.acols.at[me], PASS, partner),
        move(r.amain.at[me], r.amain.at[me], PASS, partner),
    ]
    for m in t_near:
        m.start()

    settle(r.recv.at[RAW], raw)
    relay = move(r.xtg.at[0], r.xtg.at[1], RELAY, partner)
    relay.start()

    for c in range(chunks):
        depthwise_taps(r.dww, r.taps, c, taps, True)

    for n in range(hid // BLOCK):
        lane = slice(n * BLOCK, (n + 1) * BLOCK)
        r.woutt[:, lane] = r.wout[lane].T
    for a in range(3):
        for b in range(3):
            at, flipped = (a * 3 + b) * channels, ((2 - a) * 3 + 2 - b) * channels
            r.cwt[at : at + channels] = r.cw[flipped : flipped + channels].T

    fetched("image")
    image = r.image_ref[g]
    keep = {}
    for d, near in ((1, jnp.maximum(g - 1, 0)), (0, jnp.minimum(g + 1, groups - 1))):
        there = (g > 0) if d == 1 else (g < groups - 1)
        keep[d] = (r.image_ref[near] == image).astype(jnp.float32) * there.astype(jnp.float32)

    settle(r.recv.at[RELAY], raw)
    lower = slice(upper, half)
    r.grid_g[1 + upper : half + 1, inner, :] = total_of(
        [r.gmain[0, lower]] + [ref[...] * mask for ref, mask in held_far(me)]
    )
    for side_at, who, col, at in ((0, me - 1, half - 1, PAD - 1), (1, me + 1, 0, PAD + half)):
        r.grid_g[1 + upper : half + 1, at, :] = total_of(
            [r.gcols[side_at, lower]] + [ref[:, col, :] * mask[: half - upper] for ref, mask in held_far(who)]
        )
    received_rows(GROWS)
    settle(r.recv.at[GFAR], masked)
    r.grid_g[1 : 1 + upper, inner, :] = total_of([r.gmain[0, :upper]] + [r.rmain[k] for k in range(pairs - 1)])
    for side_at, at in ((0, PAD - 1), (1, PAD + half)):
        r.grid_g[1 : 1 + upper, at, :] = total_of(
            [r.gcols[side_at, :upper]] + [r.rcols[k, side_at, :upper] for k in range(pairs - 1)]
        )
    for d, row in ((1, 0), (0, half + 1)):
        r.grid_g[row, inner, :] = total_of([r.grow[d, k] for k in range(pairs)]) * keep[d]
        corner = total_of([r.gcorn_in[d, k] for k in range(pairs)]) * keep[d]
        r.grid_g[row, PAD - 1 : PAD, :] = corner[0:1]
        r.grid_g[row, PAD + half : PAD + half + 1, :] = corner[1:2]

    for a in range(3):
        for b in range(3):
            part = r.grid_g[a : a + half, PAD - 1 + b : PAD - 1 + b + half, :]
            at = (a * 3 + b) * channels
            r.lhs[:cells, at : at + channels] = part.reshape(cells, channels).astype(jnp.bfloat16)
    grads = jnp.dot(r.lhs[:cells], r.cwt[...], preferred_element_type=jnp.float32)
    grads = grads * 0.25
    for c in range(chunks):
        lane = slice(c * LANES, (c + 1) * LANES)
        r.gq[c] = grads[:, lane].reshape(half, half, LANES)
    scaled = (grads * vector(r.scale)).astype(jnp.bfloat16)

    for n in range(hid // BLOCK):
        lane = slice(n * BLOCK, (n + 1) * BLOCK)
        dh = jnp.dot(scaled, r.woutt[:, lane], preferred_element_type=jnp.float32)
        for q in range(4):
            rows = slice(q * cells, (q + 1) * cells)
            r.dpb[rows, lane] = (dh * r.dg[rows, lane]).astype(jnp.bfloat16)
    dn_all = nt_dot(r.dpb[...], r.win[...])
    for q in range(4):
        dn = dn_all[q * cells : (q + 1) * cells] * vector(r.gain)
        parts = [dn[:, c * LANES : (c + 1) * LANES] for c in range(chunks)]
        first = jnp.sum(functools.reduce(jnp.add, parts), axis=1, keepdims=True) / channels
        cross = functools.reduce(jnp.add, [parts[c] * r.sp[c, q] for c in range(chunks)])
        second = jnp.sum(cross, axis=1, keepdims=True) / channels
        for c in range(chunks):
            back = r.rstd[q] * (parts[c] - first - r.sp[c, q] * second)
            back = back.reshape(half, half, LANES)
            for i in range(half):
                r.gpad[c, reach + 2 * i + q // 2, pl.ds(PAD + q % 2, half, stride=2), :] = back[i]

    def backward_conv(c):
        outs = depthwise(r.gpad, r.sums, r.taps, c, taps, side, True)
        for parity in range(2):
            for i in range(side):
                r.obuf[c, i, pl.ds(parity, half, stride=2), :] = outs[parity][i] + r.gq[c, i // 2]

    def pass_on(part):
        if part == 0:
            received_rows(TROWS)
            for d, dr in ((0, -1), (1, 1)):

                @pl.when(beyond[-dr])
                def _():
                    for k in range(pairs):
                        who = seat(k, 1 - core)
                        for ref in (r.arow.at[d, who], r.acorn.at[d, who]):
                            move(ref, ref, PROWS + d, partner).start()

        settle(r.recv.at[TFAR + part], main - (pairs - 1) * (tile // 2) if part == 0 else (pairs - 1) * (tile // 2))
        for k in range(1, pairs):
            who = seat(k, 1 - core)
            if part == 0:
                refs = (r.acols.at[who], r.amain.at[who, : half // 2])
            else:
                refs = (r.amain.at[who, half // 2 :],)
            for ref in refs:
                move(ref, ref, PASS, partner).start()

    pass_on(0)
    backward_conv(0)
    pass_on(1)
    backward_conv(1)
    backward_conv(2)
    chosen = [[wide(mask) for mask in masks_of(p, me)] for p in range(peers)]
    bias = vector(r.cb)

    settle(r.recv.at[PASS], main + tile + 2 * edge)
    received_rows(PROWS)

    settle(r.send.at[0], (peers - 1) * 8 * LANES + slots * tile + 2 * raw + masked + 2 * main + tile + 2 * edge)
    for d, dr in ((0, -1), (1, 1)):

        @pl.when(beyond[dr])
        def _():
            settle(r.send.at[1 + d], 2 * strips)

        @pl.when(beyond[-dr])
        def _():
            settle(r.send.at[3 + d], strips)

    for s in range(slots):
        total = None
        west = jnp.zeros((half, channels), jnp.float32)
        east = jnp.zeros((half, channels), jnp.float32)
        line = {d: jnp.zeros((half, channels), jnp.float32) for d in range(2)}
        tips = {d: [jnp.zeros((1, channels), jnp.float32) for _ in range(2)] for d in range(2)}
        for p in range(peers):
            mask = chosen[p][s]
            part = (r.amain[p] + bias) * mask
            total = part if total is None else total + part
            if p > 0:
                west = west + r.acols[p - 1, 1] * mask
            if p < peers - 1:
                east = east + r.acols[p + 1, 0] * mask
            for d in range(2):
                line[d] = line[d] + r.arow[d, p] * mask
                if p > 0:
                    tips[d][0] = tips[d][0] + r.acorn[d, p - 1, 1:2, :] * mask[:1]
                if p < peers - 1:
                    tips[d][1] = tips[d][1] + r.acorn[d, p + 1, 0:1, :] * mask[:1]
        r.tokout[s] = total
        r.tokout[s, :, 0, :] += west
        r.tokout[s, :, half - 1, :] += east
        for d, row in ((1, 0), (0, half - 1)):
            r.tokout[s, row] += line[d] * keep[d]
            r.tokout[s, row, 0:1, :] += tips[d][0] * keep[d]
            r.tokout[s, row, half - 1 : half, :] += tips[d][1] * keep[d]


def tail(obuf, tokout, tok_hbm, dx_hbm, sems):
    chunks = obuf.shape[0]
    copies = [pltpu.make_async_copy(tokout, tok_hbm, sems.at[chunks])]
    for c in range(chunks):
        copies.append(
            pltpu.make_async_copy(obuf.at[c], dx_hbm.at[:, :, c * LANES : (c + 1) * LANES], sems.at[c])
        )
    for copy in copies:
        copy.start()
    for copy in copies:
        copy.wait()


def solution(mesh):
    groups, peers = mesh.shape["group"], mesh.shape["peer"]

    def on_device(
        features, image_of_row, llm_peer, token_grads, dw_weight, dw_bias, ln_gain, ln_bias,
        w_in, b_in, w_out, b_out, layer_scale, comp_weight, comp_bias,
    ):
        side, width, channels = features.shape
        slots = token_grads.shape[0]
        hid = w_in.shape[1]
        taps = math.isqrt(dw_weight.shape[0])
        half = side // 2
        cells = half * half
        chunks = channels // LANES
        assert width == side and llm_peer.shape == (1, 1)
        assert taps == 7 and side % 4 == 0
        f32, bf16 = jnp.float32, jnp.bfloat16
        padded = (chunks, side + 2 * (taps // 2), side + 2 * PAD, LANES)
        block = (half, half, channels)
        strip = (half, channels)
        tip = (2, channels)
        hbm = pl.BlockSpec(memory_space=pltpu.HBM)
        pairs = peers // 2
        assert peers == 2 * pairs and pairs > 1
        vmem = pl.BlockSpec(memory_space=pltpu.VMEM)

        def dma(count):
            return pltpu.SemaphoreType.DMA((count,))

        def buf(*shape, kind=f32):
            return pltpu.VMEM(shape, kind)

        inputs = (
            "image_hbm", "owner_hbm", "x_hbm", "tg_hbm", "dww_hbm", "dwb_hbm", "gain_hbm", "lnb_hbm",
            "win_hbm", "bin_hbm", "wout_hbm", "bout_hbm", "scale_hbm", "cw_hbm", "cb_hbm",
        )
        held = {
            "obuf": buf(chunks, side, side, LANES),
            "tokout": buf(slots, *block),
        }
        sent = (slots + 1) * cells * channels + 2 * half * channels + peers * 8 * LANES
        sent += (pairs - 1) * (3 * (cells + 2 * half) + 3 * slots * cells) * channels
        span = max(sent, (side * side + taps * taps + 6) * channels + hid) // LANES
        scratch = {
            "xpad": buf(*padded),
            "gpad": buf(*padded),
            "sums": buf((side + taps - 1) // 2 + (side + taps - 1) // 4 * 2, side + 2 * PAD, LANES),
            "taps": buf(chunks, 2 * taps + 1, 8, LANES),
            "dww": buf(chunks, taps * taps, LANES),
            "gq": buf(chunks, half, half, LANES),
            "dwb": buf(channels),
            "gain": buf(channels),
            "lnb": buf(channels),
            "bout": buf(channels),
            "scale": buf(channels),
            "cb": buf(channels),
            "bin_": buf(hid),
            "win": buf(*w_in.shape, kind=bf16),
            "woutt": buf(channels, hid, kind=bf16),
            "wout": buf(*w_out.shape, kind=bf16),
            "cw": buf(9 * channels, channels, kind=bf16),
            "cwt": buf(9 * channels, channels, kind=bf16),
            "lhs": buf((half + 2) * WIDE, 9 * channels, kind=bf16),
            "tg": buf(slots, *block),
            "ntg": buf(slots, *block),
            "sp": buf(chunks, 4, cells, LANES),
            "rstd": buf(4, cells, LANES),
            "nb": buf(4 * cells, channels, kind=bf16),
            "dg": buf(4 * cells, hid),
            "hb": buf(cells, hid, kind=bf16),
            "dpb": buf(4 * cells, hid, kind=bf16),
            "table": buf(peers, 8, LANES, kind=jnp.int32),
            "gmain": buf(pairs, *block),
            "gcols": buf(2, *strip),
            "gfar": buf(pairs - 1, 2, half // 2, channels),
            "xtg": buf(2, pairs - 1, slots, half - half // 2, half, channels),
            "gcorn": buf(pairs, 2, *tip),
            "rmain": buf(pairs - 1, half // 2, half, channels),
            "rcols": buf(pairs - 1, 2, half // 2, channels),
            "grow": buf(2, pairs, *strip),
            "gcorn_in": buf(2, pairs, *tip),
            "grid_g": buf(half + 2, half + 2 * PAD, channels),
            "grid_p": buf(half + 4, PAD + WIDE + PAD, channels),
            "beside": buf(half + 2, WIDE - half, channels),
            "erow": buf(2, *strip),
            "ecorn": buf(2, *tip),
            "amain": buf(peers, *block),
            "acols": buf(peers, 2, *strip),
            "arow": buf(2, peers, *strip),
            "acorn": buf(2, peers, *tip),
            "image_ref": pltpu.SMEM(image_of_row.shape, jnp.int32),
            "owner_ref": pltpu.SMEM((1, 1), jnp.int32),
            "in_sems": dma(7),
            "hello": pltpu.SemaphoreType.REGULAR,
            "send": dma(5),
            "span": buf(span, 1, LANES),
            "recv": dma(13),
        }
        names = inputs + tuple(held) + tuple(scratch)
        state = pl.pallas_call(
            functools.partial(kernel, groups, peers, taps, names),
            out_shape=tuple(held.values()),
            in_specs=[hbm] * len(inputs),
            out_specs=(vmem,) * len(held),
            scratch_shapes=list(scratch.values()),
            compiler_params=pltpu.CompilerParams(collective_id=0, has_side_effects=True),
        )(
            image_of_row,
            llm_peer,
            features,
            token_grads.reshape((slots,) + block),
            dw_weight,
            dw_bias,
            ln_gain,
            ln_bias,
            w_in,
            b_in,
            w_out,
            b_out,
            layer_scale,
            comp_weight.reshape(9 * channels, channels),
            comp_bias,
        )
        tokens, grads = pl.pallas_call(
            tail,
            out_shape=(
                jax.ShapeDtypeStruct((slots,) + block, f32),
                jax.ShapeDtypeStruct(features.shape, f32),
            ),
            in_specs=[vmem] * len(held),
            out_specs=(hbm, hbm),
            scratch_shapes=[dma(chunks + 1)],
            compiler_params=pltpu.CompilerParams(vmem_limit_bytes=16 << 20),
        )(*state)
        return tokens.reshape(slots, cells, channels), grads

    placed = [P()] * 15
    placed[0] = P("group", "peer", None)
    placed[2] = P(("group", "peer"), None)
    placed[3] = P(("group", "peer"), None, None)
    return jax.shard_map(
        on_device,
        mesh=mesh,
        in_specs=tuple(placed),
        out_specs=(P(("group", "peer"), None, None), P("group", "peer", None)),
        check_vma=False,
    )
```
